256 devices in a mesh: grp: 2 (over z), cand: 128 (over x, y, core).
Axes of the slice: x: 8, y: 8, z: 2, core: 2. Of those that a mesh axis runs over, the one named last changes fastest.
The devices are a block of a 8x8x16 slice.
Arguments:
- prompt_key_rows: bfloat16 [2048, 512], P(('grp', 'cand')), parts along dimension 0, may hold values from -6 to 6
- prompt_value_rows: bfloat16 [2048, 512], P(('grp', 'cand')), parts along dimension 0, may hold values from -6 to 6
- queries: bfloat16 [32768, 4096], P(('grp', 'cand')), parts along dimension 0, may hold values from -6 to 6
- keys: bfloat16 [32768, 512], P(('grp', 'cand')), parts along dimension 0, may hold values from -6 to 6
- values: bfloat16 [32768, 512], P(('grp', 'cand')), parts along dimension 0, may hold values from -6 to 6
- output_gradient: bfloat16 [32768, 4096], P(('grp', 'cand')), parts along dimension 0, may hold values from -12 to 12
- lengths: int32 [256], P(('grp', 'cand')), parts along dimension 0, may hold values from 1 to 120, 5120 in all
- prompt_visible_rows: int32 [256], P(('grp', 'cand')), parts along dimension 0, may hold values from 256 to 1024
- query_gain: float32 [128], replicated, may hold values from 0.25 to 1.75
- key_norm_gain: float32 [128], replicated, may hold values from 0.25 to 1.75
- key_value_weight: bfloat16 [5120, 1024], P('cand'), may hold values from -0.25 to 0.25
Outputs:
- query_grad: bfloat16 [32768, 4096], P(('grp', 'cand')), parts along dimension 0
- key_grad: bfloat16 [32768, 512], P(('grp', 'cand')), parts along dimension 0
- value_grad: bfloat16 [32768, 512], P(('grp', 'cand')), parts along dimension 0
- prompt_hidden_grad: bfloat16 [2048, 5120], P(('grp', 'cand')), parts along dimension 0
The draws below stay inside these ranges and needn't reach their ends.
There are 2 independent parts, one for each index of `grp`. The reference program is written for one: setup_inputs(seed, part) draws one part's arguments, and reference() takes and returns one part's arrays. A program takes and returns all parts, laid end to end along the dimension named above; an argument that names none is the same for every part. Nothing has to cross between parts.
Inputs may be any that keep to these rules, and one draw needn't show every extreme that they name: The first lengths[c] of candidate c's 128 slots hold its response, the rest are padding.
All inputs are finite; a program needn't handle non-finite values. No bound on the sum of `lengths` on one device may be relied on, other than what follows from the above.
Results may differ from the reference program's by a relative error of at most 0.0098.
Values may be sent and summed in bfloat16 or wider, within the bound.
No kernel may reach another device: no remote copies, remote signals or barrier semaphores. Data moves between devices by JAX's collectives and lax.ppermute only.
A program may use at most 128 MiB of HBM per device.

```python
import math
import jax
import jax.numpy as jnp
import numpy as np
from jax import lax

MODEL_WIDTH = 5120
QUERY_HEADS = 32
KEY_VALUE_HEADS = 4
HEAD_WIDTH = 128
RESPONSE_SLOTS = 128
LONGEST = 120
MEAN_LEN = 40
PROMPT_ROWS = 1024
CANDIDATE_COUNT = 128


def with_ends(drawn, key, least, top_value):
    place = [jax.random.randint(jax.random.fold_in(key, axis), (), 0, length) for axis, length in enumerate(drawn.shape)]
    longest = drawn.shape.index(max(drawn.shape))
    neighbour = place[:longest] + [(place[longest] + 1) % drawn.shape[longest]] + place[longest + 1:]
    return drawn.at[tuple(place)].set(least).at[tuple(neighbour)].set(top_value)


def steps_of(rng, extent, split, low, top_value):
    level = 1.0
    for position, blocks in split:
        heights = jax.random.uniform(jax.random.fold_in(jax.random.fold_in(rng, 6), position), (blocks,), jnp.float32, low / len(split), top_value / len(split))
        level = level * jnp.repeat(jnp.exp(heights), extent[position] // blocks).reshape((-1,) + (1,) * (len(extent) - 1 - position))
    return level


def split_up(amount, total, most, skew):
    loads = [(1 << 20) // math.isqrt(standing ** skew) + 1 for standing in range(2, amount + 1)]
    surplus, holding = total - most - (amount - 1), [1] * (amount - 1)
    while surplus > 0:
        free = [i for i in range(amount - 1) if holding[i] < most]
        pool, left = sum([loads[i] for i in free]), surplus
        for i in free:
            extra = min(most - holding[i], max(1, left * loads[i] // pool), surplus)
            holding[i] = holding[i] + extra
            surplus = surplus - extra
    return np.array([most] + holding)


def ragged(own_key, amount, total, limit, skew):
    if amount == 2:
        one = jax.random.randint(own_key, (), max(1, total - limit), min(limit, total - 1) + 1)
        return jnp.stack([one, total - one])
    sizes = jnp.asarray(split_up(amount, total, limit, skew), jnp.int32)
    couples = (amount - 1) // 2
    source_of, sink = sizes[1:1 + 2 * couples:2], sizes[2:2 + 2 * couples:2]
    room = jnp.minimum(source_of - 1, limit - sink)
    passed = jax.random.randint(jax.random.fold_in(own_key, 1), (couples,), 0, 1 << 20) % (room + 1)
    sizes = sizes.at[1:1 + 2 * couples:2].set(source_of - passed).at[2:2 + 2 * couples:2].set(sink + passed)
    return sizes[jax.random.permutation(jax.random.fold_in(own_key, 2), amount)]


def scatter_about(own_key, shape, spread, bound, cuts=(), held_as=jnp.bfloat16):
    level = steps_of(own_key, shape, cuts, -0.22, 0.18) if cuts else 1.0
    result = jax.random.normal(own_key, shape, jnp.float32) * spread * level
    return jnp.minimum(jnp.maximum(result, -bound), bound).astype(held_as)


def setup_inputs(seed: int = 0, part: int = 0) -> dict:
    splits = jax.random.split(jax.random.key(seed), 12)
    part_keys = jax.random.split(jax.random.fold_in(splits[11], part), 12)
    return {
        "prompt_key_rows": scatter_about(part_keys[0], (PROMPT_ROWS, KEY_VALUE_HEADS * HEAD_WIDTH), 1.0, 6.0, ((0, 128),)),
        "prompt_value_rows": scatter_about(part_keys[1], (PROMPT_ROWS, KEY_VALUE_HEADS * HEAD_WIDTH), 1.0, 6.0, ((0, 128),)),
        "queries": scatter_about(part_keys[2], (CANDIDATE_COUNT * RESPONSE_SLOTS, QUERY_HEADS * HEAD_WIDTH), 1.0, 6.0, ((0, 128),)),
        "keys": scatter_about(part_keys[3], (CANDIDATE_COUNT * RESPONSE_SLOTS, KEY_VALUE_HEADS * HEAD_WIDTH), 1.0, 6.0, ((0, 128),)),
        "values": scatter_about(part_keys[4], (CANDIDATE_COUNT * RESPONSE_SLOTS, KEY_VALUE_HEADS * HEAD_WIDTH), 1.0, 6.0, ((0, 128),)),
        "output_gradient": scatter_about(part_keys[5], (CANDIDATE_COUNT * RESPONSE_SLOTS, QUERY_HEADS * HEAD_WIDTH), 2.0, 12.0, ((0, 128),)),
        "lengths": ragged(part_keys[6], CANDIDATE_COUNT, MEAN_LEN * CANDIDATE_COUNT, LONGEST, 2).astype(jnp.int32),
        "prompt_visible_rows": with_ends(jax.random.randint(part_keys[7], (CANDIDATE_COUNT,), PROMPT_ROWS // 4, PROMPT_ROWS + 1), jax.random.fold_in(part_keys[7], 1), PROMPT_ROWS // 4, PROMPT_ROWS).astype(jnp.int32),
        "query_gain": jnp.clip(1.0 + 0.15 * jax.random.normal(splits[8], (HEAD_WIDTH,), jnp.float32), 0.25, 1.75),
        "key_norm_gain": jnp.clip(1.0 + 0.15 * jax.random.normal(splits[9], (HEAD_WIDTH,), jnp.float32), 0.25, 1.75),
        "key_value_weight": scatter_about(splits[10], (MODEL_WIDTH, 2 * KEY_VALUE_HEADS * HEAD_WIDTH), (KEY_VALUE_HEADS * HEAD_WIDTH) ** -0.5, 0.25, ((0, 128),)),
    }


epsilon = 1e-06

def head_norm_forward(raw, gain, heads):
    count = raw.shape[0]
    inputs = raw.astype(jnp.float32).reshape(count, heads, -1)
    factor = lax.rsqrt(lax.optimization_barrier(jnp.mean(inputs * inputs, axis=-1, keepdims=True)) + epsilon)
    normed = (inputs * factor * gain).reshape(count, -1).astype(jnp.bfloat16)
    return (inputs, factor, normed)

def norm_backward(inputs, factor, gain, upstream):
    count = inputs.shape[0]
    scaled = upstream.reshape(inputs.shape) * gain
    inner = lax.optimization_barrier(jnp.mean(scaled * inputs, axis=-1, keepdims=True))
    return (factor * scaled - inputs * (factor * factor * factor) * inner).reshape(count, -1)

def contract_rows(left, right):
    return lax.dot_general(left, right, (((0,), (0,)), ((), ())), preferred_element_type=jnp.float32)

def attend(normed_q, all_keys, all_values, masked_grad, visible, head_dim):
    count = normed_q.shape[0]
    total = all_keys.shape[0]
    kv_heads = all_keys.shape[1] // head_dim
    group = normed_q.shape[1] // (kv_heads * head_dim)
    scale = head_dim ** (-0.5)
    weight_mask = visible.astype(jnp.float32)[:, None, :]
    q_parts, k_parts, v_parts = ([], [], [])
    for head in range(kv_heads):
        width = group * head_dim
        q_block = normed_q[:, head * width:(head + 1) * width].reshape(count * group, head_dim)
        g_block = masked_grad[:, head * width:(head + 1) * width].reshape(count * group, head_dim)
        k_block = all_keys[:, head * head_dim:(head + 1) * head_dim]
        v_block = all_values[:, head * head_dim:(head + 1) * head_dim]
        scores = jnp.dot(q_block, k_block.T, preferred_element_type=jnp.float32).reshape(count, group, total) * scale
        expo = jnp.exp(scores) * weight_mask
        probs = expo / lax.optimization_barrier(jnp.sum(expo, axis=-1, keepdims=True))
        probs_low = probs.astype(jnp.bfloat16).reshape(count * group, total)
        v_parts.append(contract_rows(probs_low, g_block))
        dprobs = jnp.dot(g_block, v_block.T, preferred_element_type=jnp.float32).reshape(count, group, total)
        delta = lax.optimization_barrier(jnp.sum(probs * dprobs, axis=-1, keepdims=True))
        dscore = (probs * (dprobs - delta) * scale).astype(jnp.bfloat16).reshape(count * group, total)
        q_parts.append(jnp.dot(dscore, k_block, preferred_element_type=jnp.float32).reshape(count, width))
        k_parts.append(contract_rows(dscore, q_block))
    return (jnp.concatenate(q_parts, axis=1), jnp.concatenate(k_parts, axis=1), jnp.concatenate(v_parts, axis=1))

def reference(prompt_key_rows, prompt_value_rows, queries, keys, values, output_gradient, lengths, prompt_visible_rows, query_gain, key_norm_gain, key_value_weight):
    prompt_norm_inputs, prompt_norm_factor, prompt_after_norm = head_norm_forward(prompt_key_rows, key_norm_gain, KEY_VALUE_HEADS)
    prompt_index = jnp.arange(PROMPT_ROWS, dtype=jnp.int32)
    slot_index = jnp.arange(RESPONSE_SLOTS, dtype=jnp.int32)
    causal = slot_index[None, :] <= slot_index[:, None]

    def one_candidate(carry, item_list):
        q_raw, key_before_norm, v_raw, g_raw, length, seen = item_list
        q_inputs, q_factor, q_normed = head_norm_forward(q_raw, query_gain, QUERY_HEADS)
        key_norm_inputs, key_norm_factor, key_after_norm = head_norm_forward(key_before_norm, key_norm_gain, KEY_VALUE_HEADS)
        masked_grad = jnp.where((slot_index < length)[:, None], g_raw, jnp.zeros_like(g_raw))
        prompt_visible = jnp.broadcast_to((prompt_index < seen)[None, :], (RESPONSE_SLOTS, PROMPT_ROWS))
        visible = jnp.concatenate([prompt_visible, causal], axis=1)
        all_keys = jnp.concatenate([prompt_after_norm, key_after_norm], axis=0)
        all_values = jnp.concatenate([prompt_value_rows, v_raw], axis=0)
        dq_n, dk_n, dv_n = attend(q_normed, all_keys, all_values, masked_grad, visible, HEAD_WIDTH)
        q_out = norm_backward(q_inputs, q_factor, query_gain, dq_n).astype(jnp.bfloat16)
        k_out = norm_backward(key_norm_inputs, key_norm_factor, key_norm_gain, dk_n[PROMPT_ROWS:]).astype(jnp.bfloat16)
        v_out = dv_n[PROMPT_ROWS:].astype(jnp.bfloat16)
        return ((carry[0] + dk_n[:PROMPT_ROWS], carry[1] + dv_n[:PROMPT_ROWS]), (q_out, k_out, v_out))
    zero_filled = jnp.zeros((PROMPT_ROWS, KEY_VALUE_HEADS * HEAD_WIDTH), jnp.float32)
    item_list = (queries.reshape(CANDIDATE_COUNT, RESPONSE_SLOTS, QUERY_HEADS * HEAD_WIDTH), keys.reshape(CANDIDATE_COUNT, RESPONSE_SLOTS, KEY_VALUE_HEADS * HEAD_WIDTH), values.reshape(CANDIDATE_COUNT, RESPONSE_SLOTS, KEY_VALUE_HEADS * HEAD_WIDTH), output_gradient.reshape(CANDIDATE_COUNT, RESPONSE_SLOTS, QUERY_HEADS * HEAD_WIDTH), lengths, prompt_visible_rows)
    sums, output_list = lax.scan(one_candidate, (zero_filled, zero_filled), item_list)
    prompt_dk = norm_backward(prompt_norm_inputs, prompt_norm_factor, key_norm_gain, sums[0]).astype(jnp.bfloat16)
    prompt_grads = jnp.concatenate([prompt_dk, sums[1].astype(jnp.bfloat16)], axis=1)
    hidden_state = lax.dot_general(prompt_grads, key_value_weight, (((1,), (1,)), ((), ())), preferred_element_type=jnp.float32).astype(jnp.bfloat16)
    return (output_list[0].reshape(CANDIDATE_COUNT * RESPONSE_SLOTS, QUERY_HEADS * HEAD_WIDTH), output_list[1].reshape(CANDIDATE_COUNT * RESPONSE_SLOTS, KEY_VALUE_HEADS * HEAD_WIDTH), output_list[2].reshape(CANDIDATE_COUNT * RESPONSE_SLOTS, KEY_VALUE_HEADS * HEAD_WIDTH), hidden_state)
```

```python
import functools

import jax
import jax.numpy as jnp
from jax import lax
from jax.experimental import pallas as pl
from jax.experimental.pallas import tpu as pltpu
from jax.sharding import Mesh
from jax.sharding import PartitionSpec as P

CAND = ("cand_0", "cand_1", "cand_2")
GRP_CAND = ("grp", "cand_0", "cand_1", "cand_2")
PLANE = ("cand_0", "cand_1")
FAR, NEAR, PAIR = CAND
ROW_SLOTS = 32
KEY_CHUNK = 128
LOG2_E = 1.4426950408889634

epsilon = 1e-06


def swap(x):
    return lax.ppermute(x, PAIR, [(0, 1), (1, 0)])


def from_everyone(shard, axis):
    copies = jnp.broadcast_to(shard, (lax.axis_size(axis), *shard.shape))
    return lax.all_to_all(copies, axis, split_axis=0, concat_axis=0, tiled=True)


def contract_last(left, right):
    return lax.dot_general(
        left, right, (((1,), (1,)), ((), ())), preferred_element_type=jnp.float32
    )


def contract_first(left, right):
    return lax.dot_general(
        left, right, (((0,), (0,)), ((), ())), preferred_element_type=jnp.float32
    )


def head_kernel(
    meta,
    q_own, g_own, k_own, v_own,
    q_other, g_other, k_other, v_other,
    prompt,
    q_gain, k_gain,
    dq_own, dk_own, dv_own, dq_other, dk_other, dv_other, prompt_grads,
    kn, vv, x_s, r_s, qs, gs, e_s, dp_s, ds_s, dk_acc, dv_acc,
):
    slots, width = q_own.shape
    head_dim = k_own.shape[1]
    group = width // head_dim
    prompt_total = prompt.shape[0]
    total = prompt_total + slots
    rows = ROW_SLOTS * group
    scale = head_dim ** (-0.5)
    gain_q, gain_k = q_gain[...], k_gain[...]

    kn[:prompt_total] = prompt[:, :head_dim]
    vv[:prompt_total] = prompt[:, head_dim:]
    dk_acc[:prompt_total] = jnp.zeros((prompt_total, head_dim), jnp.float32)
    dv_acc[:prompt_total] = jnp.zeros((prompt_total, head_dim), jnp.float32)

    units = (
        (0, q_own, g_own, k_own, v_own, dq_own, dk_own, dv_own),
        (1, q_other, g_other, k_other, v_other, dq_other, dk_other, dv_other),
    )
    for which, q_ref, g_ref, k_ref, v_ref, dq_ref, dk_ref, dv_ref in units:
        length, seen = meta[2 * which], meta[2 * which + 1]
        key_x = k_ref[...].astype(jnp.float32)
        key_r = lax.rsqrt(jnp.mean(key_x * key_x, axis=-1, keepdims=True) + epsilon)
        kn[prompt_total:] = (key_x * key_r * gain_k).astype(jnp.bfloat16)
        vv[prompt_total:] = v_ref[...]
        dk_acc[prompt_total:] = jnp.zeros((slots, head_dim), jnp.float32)
        dv_acc[prompt_total:] = jnp.zeros((slots, head_dim), jnp.float32)
        dq_ref[...] = jnp.zeros(dq_ref.shape, dq_ref.dtype)

        def row_block(b, carry, length=length, seen=seen, q_ref=q_ref, g_ref=g_ref, dq_ref=dq_ref):
            first = pl.multiple_of(b * ROW_SLOTS, ROW_SLOTS)
            at = pl.ds(first, ROW_SLOTS)
            live = (
                lax.broadcasted_iota(jnp.int32, (ROW_SLOTS, head_dim), 0) + first < length
            )
            for g in range(group):
                cols = slice(g * head_dim, (g + 1) * head_dim)
                mine = slice(g * ROW_SLOTS, (g + 1) * ROW_SLOTS)
                x = q_ref[at, cols].astype(jnp.float32)
                r = lax.rsqrt(jnp.mean(x * x, axis=-1, keepdims=True) + epsilon)
                x_s[mine] = x
                r_s[mine] = jnp.broadcast_to(r, x.shape)
                qs[mine] = (x * r * gain_q).astype(jnp.bfloat16)
                grad = g_ref[at, cols].astype(jnp.float32)
                gs[mine] = jnp.where(live, grad, 0.0).astype(jnp.bfloat16)
            q, go = qs[...], gs[...]
            sums = jnp.zeros((8, rows), jnp.float32)
            dots = jnp.zeros((8, rows), jnp.float32)
            for base in range(0, total, KEY_CHUNK):
                chunk = slice(base, base + KEY_CHUNK)
                index = lax.broadcasted_iota(jnp.int32, (KEY_CHUNK, rows), 0)
                if base < prompt_total:
                    visible = index < seen - base
                else:
                    slot = lax.broadcasted_iota(jnp.int32, (KEY_CHUNK, rows), 1)
                    slot = (slot & (ROW_SLOTS - 1)) + first
                    visible = index + (base - prompt_total) <= slot
                s = contract_last(kn[chunk], q)
                e = jnp.where(visible, jnp.exp2(s * (scale * LOG2_E)), 0.0)
                dp = contract_last(vv[chunk], go)
                e_s[chunk] = e
                dp_s[chunk] = dp
                sums += jnp.sum(e.reshape(KEY_CHUNK // 8, 8, rows), axis=0)
                dots += jnp.sum((e * dp).reshape(KEY_CHUNK // 8, 8, rows), axis=0)
            inverse = 1.0 / jnp.sum(sums, axis=0, keepdims=True)
            delta = jnp.sum(dots, axis=0, keepdims=True) * inverse
            for base in range(0, total, KEY_CHUNK):
                chunk = slice(base, base + KEY_CHUNK)
                p = e_s[chunk] * inverse
                ds = (p * (dp_s[chunk] - delta)).astype(jnp.bfloat16)
                ds_s[chunk] = ds
                dv_acc[chunk] += jnp.dot(
                    p.astype(jnp.bfloat16), go, preferred_element_type=jnp.float32
                )
                dk_acc[chunk] += jnp.dot(ds, q, preferred_element_type=jnp.float32)
            dq = contract_first(ds_s[...], kn[...]) * scale
            x, r = x_s[...], r_s[...]
            w = dq * gain_q
            inner = jnp.mean(w * x, axis=-1, keepdims=True)
            dx = (r * w - x * (r * r * r) * inner).astype(jnp.bfloat16)
            for g in range(group):
                dq_ref[at, g * head_dim : (g + 1) * head_dim] = dx[
                    g * ROW_SLOTS : (g + 1) * ROW_SLOTS
                ]
            return carry

        lax.fori_loop(0, (length + (ROW_SLOTS - 1)) // ROW_SLOTS, row_block, 0)
        w = dk_acc[prompt_total:] * scale * gain_k
        inner = jnp.mean(w * key_x, axis=-1, keepdims=True)
        dk_ref[...] = (key_r * w - key_x * (key_r * key_r * key_r) * inner).astype(jnp.bfloat16)
        dv_ref[...] = dv_acc[prompt_total:].astype(jnp.bfloat16)
    prompt_grads[:, :head_dim] = (dk_acc[:prompt_total] * scale).astype(jnp.bfloat16)
    prompt_grads[:, head_dim:] = dv_acc[:prompt_total].astype(jnp.bfloat16)


def attend(heads, meta, own, other, prompt, q_gain, k_gain, width, head_dim):
    slots, total = own.shape[0], prompt.shape[0]
    keys = total + slots
    group = width // head_dim
    rows = ROW_SLOTS * group
    narrow = 2 * heads * group

    def columns(block, index):
        return pl.BlockSpec((slots, block), lambda i, index=index: (0, index + i))

    def by_head(rows, block):
        return pl.BlockSpec((rows, block), lambda i: (0, i))

    def whole(shape):
        return pl.BlockSpec(shape, lambda i: (0, 0))

    side = [
        columns(width, 0),
        columns(width, heads),
        columns(head_dim, narrow),
        columns(head_dim, narrow + heads),
    ]
    low = jnp.bfloat16
    outs = [(slots, width), (slots, head_dim), (slots, head_dim)] * 2 + [(total, 2 * head_dim)]
    work = heads * 2 * 5 * 2 * slots * group * keys * head_dim
    return pl.pallas_call(
        head_kernel,
        grid=(heads,),
        in_specs=[pl.BlockSpec(memory_space=pltpu.SMEM)]
        + side
        + side
        + [by_head(total, 2 * head_dim), whole((1, head_dim)), whole((1, head_dim))],
        out_specs=[by_head(*s) for s in outs],
        out_shape=[jax.ShapeDtypeStruct((n, heads * m), low) for n, m in outs],
        scratch_shapes=[
            pltpu.VMEM((keys, head_dim), low),
            pltpu.VMEM((keys, head_dim), low),
            pltpu.VMEM((rows, head_dim), jnp.float32),
            pltpu.VMEM((rows, head_dim), jnp.float32),
            pltpu.VMEM((rows, head_dim), low),
            pltpu.VMEM((rows, head_dim), low),
            pltpu.VMEM((keys, rows), jnp.float32),
            pltpu.VMEM((keys, rows), jnp.float32),
            pltpu.VMEM((keys, rows), low),
            pltpu.VMEM((keys, head_dim), jnp.float32),
            pltpu.VMEM((keys, head_dim), jnp.float32),
        ],
        compiler_params=pltpu.CompilerParams(vmem_limit_bytes=24 * 1024 * 1024),
        cost_estimate=pl.CostEstimate(
            flops=work, bytes_accessed=heads * 4 * 1024 * 1024,
            transcendentals=heads * 2 * slots * group * keys,
        ),
    )(meta, own, own, own, own, other, other, other, other, prompt, q_gain, k_gain)


def on_device(
    prompt_key_rows,
    prompt_value_rows,
    queries,
    keys,
    values,
    output_gradient,
    lengths,
    prompt_visible_rows,
    query_gain,
    key_norm_gain,
    key_value_weight,
):
    head_dim = query_gain.shape[0]
    core = lax.axis_index(PAIR)
    cores = lax.axis_size(PAIR)
    heads = keys.shape[1] // head_dim // cores
    narrow = heads * head_dim
    wide = queries.shape[1] // cores
    width = wide // heads
    near, far = lax.axis_size(NEAR), lax.axis_size(FAR)
    q_gain, k_gain = query_gain[None, :], key_norm_gain[None, :]

    def part(a, which, n):
        return lax.dynamic_slice_in_dim(a, which * n, n, axis=1)

    def in_core_order(mine, theirs):
        flip = core == 0
        return jnp.where(flip, mine, theirs), jnp.where(flip, theirs, mine)

    def prompt_part(which):
        return jnp.concatenate(
            [part(prompt_key_rows, which, narrow), part(prompt_value_rows, which, narrow)], axis=1
        )

    def pack(which):
        return jnp.concatenate(
            [
                part(queries, which, wide),
                part(output_gradient, which, wide),
                part(keys, which, narrow),
                part(values, which, narrow),
            ],
            axis=1,
        )

    def weight_part(which):
        cut = key_value_weight.reshape(-1, 2, cores, heads, head_dim)
        cut = lax.dynamic_index_in_dim(cut, which, 2, keepdims=False)
        return cut.transpose(0, 2, 1, 3).reshape(-1, 2 * narrow)

    raw = jnp.concatenate(in_core_order(prompt_part(core), swap(prompt_part(1 - core))), axis=0)
    count = raw.shape[0]
    px = raw[:, :narrow].astype(jnp.float32).reshape(count, heads, head_dim)
    pr = lax.rsqrt(jnp.mean(px * px, axis=-1, keepdims=True) + epsilon)
    pn = (px * pr * key_norm_gain).astype(jnp.bfloat16).reshape(count, narrow)
    pv = raw[:, narrow:]

    meta_own = jnp.stack([lengths[0], prompt_visible_rows[0]])
    meta = jnp.concatenate([meta_own, swap(meta_own)])
    own, other = pack(core), swap(pack(1 - core))
    weight_pair = jnp.concatenate(
        in_core_order(weight_part(core), swap(weight_part(1 - core))), axis=0
    )

    both = jnp.concatenate(
        [
            a[:, h * head_dim : (h + 1) * head_dim]
            for h in range(heads)
            for a in (pn, pv)
        ],
        axis=1,
    )
    prompt = from_everyone(both, PLANE).reshape(-1, 2 * narrow)
    weight = from_everyone(weight_pair, FAR).reshape(-1, 2 * narrow)

    results = attend(heads, meta, own, other, prompt, q_gain, k_gain, width, head_dim)

    sent = results[6].reshape(far * near, count, 2 * narrow)
    parts = lax.all_to_all(sent, PLANE, 0, 0, tiled=True)
    total = jnp.sum(parts.astype(jnp.float32), axis=0).reshape(count, heads, 2, head_dim)
    w = total[:, :, 0] * key_norm_gain
    inner = jnp.mean(w * px, axis=-1, keepdims=True)
    dk = pr * w - px * (pr * pr * pr) * inner
    grads = jnp.stack([dk, total[:, :, 1]], axis=2).reshape(count, 2 * narrow)
    rows = from_everyone(grads.astype(jnp.bfloat16), NEAR).reshape(-1, 2 * narrow)

    def assembled(index):
        return jnp.concatenate(in_core_order(results[index], swap(results[index + 3])), axis=1)

    query_grad, key_grad, value_grad = assembled(0), assembled(1), assembled(2)

    hidden = contract_last(rows, weight)
    per_core = count // cores
    hidden = hidden.reshape(near, cores, per_core, -1)
    mine = lax.dynamic_index_in_dim(hidden, core, 1, keepdims=False)
    theirs = lax.dynamic_index_in_dim(hidden, 1 - core, 1, keepdims=False)
    mine = (mine + swap(theirs.astype(jnp.bfloat16)).astype(jnp.float32)).astype(jnp.bfloat16)
    arrived = lax.all_to_all(mine, NEAR, 0, 0, tiled=True)
    arrived = arrived.reshape(near, per_core, far, -1)
    hidden_grad = arrived.transpose(1, 2, 0, 3).reshape(per_core, -1)
    return (query_grad, key_grad, value_grad, hidden_grad)


def solution(mesh):
    finer = Mesh(
        mesh.devices.reshape(mesh.shape["grp"], 8, 8, 2), ("grp", "cand_0", "cand_1", "cand_2")
    )
    return jax.shard_map(
        on_device,
        mesh=finer,
        in_specs=(
            P(GRP_CAND, None),
            P(GRP_CAND, None),
            P(GRP_CAND, None),
            P(GRP_CAND, None),
            P(GRP_CAND, None),
            P(GRP_CAND, None),
            P(GRP_CAND),
            P(GRP_CAND),
            P(),
            P(),
            P(CAND, None),
        ),
        out_specs=(P(GRP_CAND, None), P(GRP_CAND, None), P(GRP_CAND, None), P(GRP_CAND, None)),
        check_vma=False,
    )
```

```python
import functools

import jax
import jax.numpy as jnp
from jax import lax
from jax.experimental import pallas as pl
from jax.experimental.pallas import tpu as pltpu
from jax.sharding import Mesh
from jax.sharding import PartitionSpec as P

CAND = ("cand_0", "cand_1", "cand_2")
GRP_CAND = ("grp", "cand_0", "cand_1", "cand_2")
PLANE = ("cand_0", "cand_1")
FAR, NEAR, PAIR = CAND
ROW_SLOTS = 32
KEY_CHUNK = 128
KEY_STEPS = 4
LOG2_E = 1.4426950408889634

epsilon = 1e-06


def swap(x):
    return lax.ppermute(x, PAIR, [(0, 1), (1, 0)])


def from_everyone(shard, axis):
    copies = jnp.broadcast_to(shard, (lax.axis_size(axis), *shard.shape))
    return lax.all_to_all(copies, axis, split_axis=0, concat_axis=0, tiled=True)


def contract_last(left, right):
    return lax.dot_general(
        left, right, (((1,), (1,)), ((), ())), preferred_element_type=jnp.float32
    )


def contract_first(left, right):
    return lax.dot_general(
        left, right, (((0,), (0,)), ((), ())), preferred_element_type=jnp.float32
    )


def head_norm(x, gain):
    r = lax.rsqrt(jnp.mean(x * x, axis=-1, keepdims=True) + epsilon)
    return r, (x * r * gain).astype(jnp.bfloat16)


def norm_backward(x, r, gain, upstream):
    w = upstream * gain
    inner = jnp.mean(w * x, axis=-1, keepdims=True)
    return r * w - x * (r * r * r) * inner


def block_count(length):
    return (length + (ROW_SLOTS - 1)) // ROW_SLOTS


def folded(x):
    return jnp.sum(x.reshape(-1, 8, x.shape[-1]), axis=0)


def causal(keys, rows, first):
    slot = lax.broadcasted_iota(jnp.int32, (keys, rows), 1) & (ROW_SLOTS - 1)
    return lax.broadcasted_iota(jnp.int32, (keys, rows), 0) <= slot + first


def exponent(k, q):
    return jnp.exp2(contract_last(k, q) * (k.shape[-1] ** (-0.5) * LOG2_E))


def before_kernel(
    meta, q_own, g_own, k_own, v_own, q_other, g_other, k_other, v_other, q_gain, k_gain,
    qs, gs, partial,
):
    slots, width = q_own.shape
    head_dim = k_own.shape[1]
    group = width // head_dim
    rows = ROW_SLOTS * group
    gain_q, gain_k = q_gain[...], k_gain[...]
    units = ((q_own, g_own, k_own, v_own), (q_other, g_other, k_other, v_other))
    for which, (q_ref, g_ref, k_ref, v_ref) in enumerate(units):
        length = meta[2 * which]
        _, kn = head_norm(k_ref[...].astype(jnp.float32), gain_k)

        def row_block(b, carry, which=which, q_ref=q_ref, g_ref=g_ref, v_ref=v_ref, kn=kn, length=length):
            first = pl.multiple_of(b * ROW_SLOTS, ROW_SLOTS)
            at = pl.ds(first, ROW_SLOTS)
            out = pl.multiple_of(b * rows, rows)
            live = lax.broadcasted_iota(jnp.int32, (ROW_SLOTS, head_dim), 0) + first < length
            normed, grads = [], []
            for g in range(group):
                cols = slice(g * head_dim, (g + 1) * head_dim)
                normed.append(head_norm(q_ref[at, cols].astype(jnp.float32), gain_q)[1])
                grad = g_ref[at, cols].astype(jnp.float32)
                grads.append(jnp.where(live, grad, 0.0).astype(jnp.bfloat16))
            q, go = jnp.concatenate(normed, axis=0), jnp.concatenate(grads, axis=0)
            qs[0, which, pl.ds(out, rows), :] = q
            gs[0, which, pl.ds(out, rows), :] = go
            e = jnp.where(causal(slots, rows, first), exponent(kn, q), 0.0)
            stats = pl.multiple_of(b * 16, 16)
            partial[0, which, pl.ds(stats, 8), :] = folded(e)
            partial[0, which, pl.ds(stats + 8, 8), :] = folded(e * contract_last(v_ref[...], go))
            return carry

        lax.fori_loop(0, block_count(length), row_block, 0)


def prompt_kernel(
    meta, prompt, qs, gs, partial, ds_out, stats, prompt_grads, e_s, dp_s, dk_acc, dv_acc
):
    total = prompt.shape[0]
    head_dim = qs.shape[-1]
    rows = e_s.shape[1]
    which = pl.program_id(1)
    length, seen = meta[2 * which], meta[2 * which + 1]

    @pl.when(which == 0)
    def _():
        dk_acc[...] = jnp.zeros(dk_acc.shape, jnp.float32)
        dv_acc[...] = jnp.zeros(dv_acc.shape, jnp.float32)

    def blocks(low, high):
        def row_block(b, carry):
            at = pl.ds(pl.multiple_of(b * rows, rows), rows)
            q, go = qs[0, 0, at, :], gs[0, 0, at, :]
            part = pl.multiple_of(b * 16, 16)
            sums = partial[0, 0, pl.ds(part, 8), :]
            dots = partial[0, 0, pl.ds(part + 8, 8), :]
            for base in range(0, high, KEY_CHUNK):
                chunk = slice(base, base + KEY_CHUNK)
                e = exponent(prompt[chunk, :head_dim], q)
                if base + KEY_CHUNK > low:
                    index = lax.broadcasted_iota(jnp.int32, (KEY_CHUNK, rows), 0)
                    e = jnp.where(index < seen - base, e, 0.0)
                dp = contract_last(prompt[chunk, head_dim:], go)
                e_s[chunk] = e
                dp_s[chunk] = dp
                sums += folded(e)
                dots += folded(e * dp)
            inverse = 1.0 / jnp.sum(sums, axis=0, keepdims=True)
            delta = jnp.sum(dots, axis=0, keepdims=True) * inverse
            stats[0, 0, pl.ds(part, 8), :] = jnp.broadcast_to(inverse, (8, rows))
            stats[0, 0, pl.ds(part + 8, 8), :] = jnp.broadcast_to(delta, (8, rows))
            for base in range(0, high, KEY_CHUNK):
                chunk = slice(base, base + KEY_CHUNK)
                p = e_s[chunk] * inverse
                ds = (p * (dp_s[chunk] - delta)).astype(jnp.bfloat16)
                ds_out[0, 0, b, chunk, :] = ds
                dv_acc[chunk] += jnp.dot(
                    p.astype(jnp.bfloat16), go, preferred_element_type=jnp.float32
                )
                dk_acc[chunk] += jnp.dot(ds, q, preferred_element_type=jnp.float32)
            return carry

        lax.fori_loop(0, block_count(length), row_block, 0)

    step = total // KEY_STEPS
    for n in range(1, KEY_STEPS + 1):
        low, high = (n - 1) * step, n * step
        pl.when((seen > low) & (seen <= high))(functools.partial(blocks, low, high))

    @pl.when(which == pl.num_programs(1) - 1)
    def _():
        scale = head_dim ** (-0.5)
        prompt_grads[:, :head_dim] = (dk_acc[...] * scale).astype(jnp.bfloat16)
        prompt_grads[:, head_dim:] = dv_acc[...].astype(jnp.bfloat16)


def after_kernel(
    meta, q_own, k_own, v_own, q_other, k_other, v_other, prompt, qs, gs, ds_in, stats,
    q_gain, k_gain,
    dq_own, dk_own, dv_own, dq_other, dk_other, dv_other, dk_acc, dv_acc,
):
    slots, width = q_own.shape
    head_dim = k_own.shape[1]
    group = width // head_dim
    rows = ROW_SLOTS * group
    total = prompt.shape[0]
    scale = head_dim ** (-0.5)
    gain_q, gain_k = q_gain[...], k_gain[...]
    units = (
        (q_own, k_own, v_own, dq_own, dk_own, dv_own),
        (q_other, k_other, v_other, dq_other, dk_other, dv_other),
    )
    for which, (q_ref, k_ref, v_ref, dq_ref, dk_ref, dv_ref) in enumerate(units):
        length, seen = meta[2 * which], meta[2 * which + 1]
        key_x = k_ref[...].astype(jnp.float32)
        key_r, kn = head_norm(key_x, gain_k)
        dq_ref[...] = jnp.zeros(dq_ref.shape, dq_ref.dtype)
        dk_acc[...] = jnp.zeros(dk_acc.shape, jnp.float32)
        dv_acc[...] = jnp.zeros(dv_acc.shape, jnp.float32)

        def blocks(high, which=which, q_ref=q_ref, v_ref=v_ref, dq_ref=dq_ref, kn=kn, length=length):
            def row_block(b, carry):
                first = pl.multiple_of(b * ROW_SLOTS, ROW_SLOTS)
                at = pl.ds(pl.multiple_of(b * rows, rows), rows)
                q, go = qs[0, which, at, :], gs[0, which, at, :]
                part = pl.multiple_of(b * 16, 16)
                inverse = stats[0, which, pl.ds(part, 8), :][:1]
                delta = stats[0, which, pl.ds(part + 8, 8), :][:1]
                e = jnp.where(causal(slots, rows, first), exponent(kn, q), 0.0)
                p = e * inverse
                ds = (p * (contract_last(v_ref[...], go) - delta)).astype(jnp.bfloat16)
                dv_acc[...] += jnp.dot(
                    p.astype(jnp.bfloat16), go, preferred_element_type=jnp.float32
                )
                dk_acc[...] += jnp.dot(ds, q, preferred_element_type=jnp.float32)
                dq = contract_first(ds, kn) + contract_first(
                    ds_in[0, which, b, :high, :], prompt[:high, :head_dim]
                )
                dq = dq * scale
                for g in range(group):
                    cols = slice(g * head_dim, (g + 1) * head_dim)
                    x = q_ref[pl.ds(first, ROW_SLOTS), cols].astype(jnp.float32)
                    r = lax.rsqrt(jnp.mean(x * x, axis=-1, keepdims=True) + epsilon)
                    up = dq[g * ROW_SLOTS : (g + 1) * ROW_SLOTS]
                    dx = norm_backward(x, r, gain_q, up)
                    dq_ref[pl.ds(first, ROW_SLOTS), cols] = dx.astype(jnp.bfloat16)
                return carry

            lax.fori_loop(0, block_count(length), row_block, 0)

        step = total // KEY_STEPS
        for n in range(1, KEY_STEPS + 1):
            low, high = (n - 1) * step, n * step
            pl.when((seen > low) & (seen <= high))(functools.partial(blocks, high))
        dk = norm_backward(key_x, key_r, gain_k, dk_acc[...] * scale)
        dk_ref[...] = dk.astype(jnp.bfloat16)
        dv_ref[...] = dv_acc[...].astype(jnp.bfloat16)


def attend(heads, meta, own, other, prompt, weight_pair, q_gain, k_gain, width, head_dim):
    slots, total = own.shape[0], prompt.shape[0]
    group = width // head_dim
    rows = ROW_SLOTS * group
    steps = slots // ROW_SLOTS
    narrow = 2 * heads * group
    low, high = jnp.bfloat16, jnp.float32
    scalars = pl.BlockSpec(memory_space=pltpu.SMEM)
    gain = pl.BlockSpec((1, head_dim), lambda *i: (0, 0))

    def columns(block, index):
        return pl.BlockSpec((slots, block), lambda i, index=index: (0, index + i))

    def by_head(rows, block):
        return pl.BlockSpec((rows, block), lambda i, *_: (0, i))

    def by_pair(*shape):
        return pl.BlockSpec((1, 2, *shape), lambda i: (i, 0) + (0,) * len(shape))

    def by_unit(*shape):
        return pl.BlockSpec((1, 1, *shape), lambda i, k: (i, k) + (0,) * len(shape))

    def cost(products, keys, moved):
        return pl.CostEstimate(
            flops=heads * 2 * products * 2 * slots * group * keys * head_dim,
            bytes_accessed=moved,
            transcendentals=heads * 2 * slots * group * keys,
        )

    q_side = columns(width, 0)
    g_side = columns(width, heads)
    k_side = columns(head_dim, narrow)
    v_side = columns(head_dim, narrow + heads)
    stack, stat, shade = (steps * rows, head_dim), (steps * 16, rows), (steps, total, rows)

    def limit(mebibytes):
        return pltpu.CompilerParams(vmem_limit_bytes=mebibytes * 1024 * 1024)

    def shaped(shape, kind):
        return jax.ShapeDtypeStruct((heads, 2, *shape), kind)

    qs, gs, partial = pl.pallas_call(
        before_kernel,
        grid=(heads,),
        in_specs=[scalars, q_side, g_side, k_side, v_side, q_side, g_side, k_side, v_side, gain, gain],
        out_specs=[by_pair(*stack), by_pair(*stack), by_pair(*stat)],
        out_shape=[shaped(stack, low), shaped(stack, low), shaped(stat, high)],
        compiler_params=limit(8),
        cost_estimate=cost(2, slots, 4 * 1024 * 1024),
    )(meta, own, own, own, own, other, other, other, other, q_gain, k_gain)
    weight_pair, prompt, qs, gs, partial = lax.optimization_barrier(
        (weight_pair, prompt, qs, gs, partial)
    )
    weight = from_everyone(weight_pair, FAR).reshape(-1, weight_pair.shape[1])
    ds, stats, prompt_grads = pl.pallas_call(
        prompt_kernel,
        grid=(heads, 2),
        in_specs=[scalars, by_head(total, 2 * head_dim), by_unit(*stack), by_unit(*stack), by_unit(*stat)],
        out_specs=[by_unit(*shade), by_unit(*stat), by_head(total, 2 * head_dim)],
        out_shape=[
            shaped(shade, low),
            shaped(stat, high),
            jax.ShapeDtypeStruct((total, heads * 2 * head_dim), low),
        ],
        scratch_shapes=[
            pltpu.VMEM((total, rows), high),
            pltpu.VMEM((total, rows), high),
            pltpu.VMEM((total, head_dim), high),
            pltpu.VMEM((total, head_dim), high),
        ],
        compiler_params=limit(57),
        cost_estimate=cost(4, total, 12 * 1024 * 1024),
    )(meta, prompt, qs, gs, partial)
    outs = [(slots, width), (slots, head_dim), (slots, head_dim)] * 2
    grads = pl.pallas_call(
        after_kernel,
        grid=(heads,),
        in_specs=[scalars, q_side, k_side, v_side, q_side, k_side, v_side]
        + [by_head(total, 2 * head_dim), by_pair(*stack), by_pair(*stack)]
        + [by_pair(*shade), by_pair(*stat), gain, gain],
        out_specs=[by_head(*s) for s in outs],
        out_shape=[jax.ShapeDtypeStruct((n, heads * m), low) for n, m in outs],
        scratch_shapes=[pltpu.VMEM((slots, head_dim), high), pltpu.VMEM((slots, head_dim), high)],
        compiler_params=limit(57),
        cost_estimate=cost(2, total, 14 * 1024 * 1024),
    )(meta, own, own, own, other, other, other, prompt, qs, gs, ds, stats, q_gain, k_gain)
    return (*grads, prompt_grads, weight)


def on_device(
    prompt_key_rows,
    prompt_value_rows,
    queries,
    keys,
    values,
    output_gradient,
    lengths,
    prompt_visible_rows,
    query_gain,
    key_norm_gain,
    key_value_weight,
):
    head_dim = query_gain.shape[0]
    core = lax.axis_index(PAIR)
    cores = lax.axis_size(PAIR)
    heads = keys.shape[1] // head_dim // cores
    narrow = heads * head_dim
    wide = queries.shape[1] // cores
    width = wide // heads
    near, far = lax.axis_size(NEAR), lax.axis_size(FAR)
    q_gain, k_gain = query_gain[None, :], key_norm_gain[None, :]

    def part(a, which, n):
        return lax.dynamic_slice_in_dim(a, which * n, n, axis=1)

    def in_core_order(mine, theirs):
        flip = core == 0
        return jnp.where(flip, mine, theirs), jnp.where(flip, theirs, mine)

    def prompt_part(which):
        return jnp.concatenate(
            [part(prompt_key_rows, which, narrow), part(prompt_value_rows, which, narrow)], axis=1
        )

    def pack(which):
        return jnp.concatenate(
            [
                part(queries, which, wide),
                part(output_gradient, which, wide),
                part(keys, which, narrow),
                part(values, which, narrow),
            ],
            axis=1,
        )

    def weight_part(which):
        cut = key_value_weight.reshape(-1, 2, cores, heads, head_dim)
        cut = lax.dynamic_index_in_dim(cut, which, 2, keepdims=False)
        return cut.transpose(0, 2, 1, 3).reshape(-1, 2 * narrow)

    raw = jnp.concatenate(in_core_order(prompt_part(core), swap(prompt_part(1 - core))), axis=0)
    count = raw.shape[0]
    px = raw[:, :narrow].astype(jnp.float32).reshape(count, heads, head_dim)
    pr = lax.rsqrt(jnp.mean(px * px, axis=-1, keepdims=True) + epsilon)
    pn = (px * pr * key_norm_gain).astype(jnp.bfloat16).reshape(count, narrow)
    pv = raw[:, narrow:]

    meta_own = jnp.stack([lengths[0], prompt_visible_rows[0]])
    meta = jnp.concatenate([meta_own, swap(meta_own)])
    own, other = pack(core), swap(pack(1 - core))
    weight_pair = jnp.concatenate(
        in_core_order(weight_part(core), swap(weight_part(1 - core))), axis=0
    )

    both = jnp.concatenate(
        [
            a[:, h * head_dim : (h + 1) * head_dim]
            for h in range(heads)
            for a in (pn, pv)
        ],
        axis=1,
    )
    prompt = from_everyone(both, PLANE).reshape(-1, 2 * narrow)

    results = attend(
        heads, meta, own, other, prompt, weight_pair, q_gain, k_gain, width, head_dim
    )

    sent, weight = lax.optimization_barrier((results[6], results[7]))
    sent = sent.reshape(far * near, count, 2 * narrow)
    parts = lax.all_to_all(sent, PLANE, 0, 0, tiled=True)
    total = jnp.sum(parts.astype(jnp.float32), axis=0).reshape(count, heads, 2, head_dim)
    w = total[:, :, 0] * key_norm_gain
    inner = jnp.mean(w * px, axis=-1, keepdims=True)
    dk = pr * w - px * (pr * pr * pr) * inner
    grads = jnp.stack([dk, total[:, :, 1]], axis=2).reshape(count, 2 * narrow)
    rows = from_everyone(grads.astype(jnp.bfloat16), NEAR).reshape(-1, 2 * narrow)

    def assembled(index):
        return jnp.concatenate(in_core_order(results[index], swap(results[index + 3])), axis=1)

    query_grad, key_grad, value_grad = assembled(0), assembled(1), assembled(2)

    hidden = contract_last(rows, weight)
    per_core = count // cores
    hidden = hidden.reshape(near, cores, per_core, -1)
    mine = lax.dynamic_index_in_dim(hidden, core, 1, keepdims=False)
    theirs = lax.dynamic_index_in_dim(hidden, 1 - core, 1, keepdims=False)
    mine = (mine + swap(theirs.astype(jnp.bfloat16)).astype(jnp.float32)).astype(jnp.bfloat16)
    arrived = lax.all_to_all(mine, NEAR, 0, 0, tiled=True)
    arrived = arrived.reshape(near, per_core, far, -1)
    hidden_grad = arrived.transpose(1, 2, 0, 3).reshape(per_core, -1)
    return (query_grad, key_grad, value_grad, hidden_grad)


def solution(mesh):
    finer = Mesh(
        mesh.devices.reshape(mesh.shape["grp"], 8, 8, 2), ("grp", "cand_0", "cand_1", "cand_2")
    )
    return jax.shard_map(
        on_device,
        mesh=finer,
        in_specs=(
            P(GRP_CAND, None),
            P(GRP_CAND, None),
            P(GRP_CAND, None),
            P(GRP_CAND, None),
            P(GRP_CAND, None),
            P(GRP_CAND, None),
            P(GRP_CAND),
            P(GRP_CAND),
            P(),
            P(),
            P(CAND, None),
        ),
        out_specs=(P(GRP_CAND, None), P(GRP_CAND, None), P(GRP_CAND, None), P(GRP_CAND, None)),
        check_vma=False,
    )
```

```python
import functools

import jax
import jax.numpy as jnp
from jax import lax
from jax.experimental import pallas as pl
from jax.experimental.pallas import tpu as pltpu
from jax.sharding import Mesh
from jax.sharding import PartitionSpec as P


CAND = ("cand_0", "cand_1", "cand_2")
GRP_CAND = ("grp", "cand_0", "cand_1", "cand_2")
PLANE = ("cand_0", "cand_1")
FAR, NEAR, PAIR = CAND
ROW_SLOTS = 32
KEY_CHUNK = 128
KEY_STEPS = 4
LOG2_E = 1.4426950408889634

epsilon = 1e-06


def swap(x):
    return lax.ppermute(x, PAIR, [(0, 1), (1, 0)])


def shifted(x, by):
    n = lax.axis_size(FAR)
    return lax.ppermute(x, FAR, [(i, (i + by) % n) for i in range(n)])


def from_everyone(shard, axis):
    copies = jnp.broadcast_to(shard, (lax.axis_size(axis), *shard.shape))
    return lax.all_to_all(copies, axis, split_axis=0, concat_axis=0, tiled=True)


def contract_last(left, right):
    return lax.dot_general(
        left, right, (((1,), (1,)), ((), ())), preferred_element_type=jnp.float32
    )


def contract_first(left, right):
    return lax.dot_general(
        left, right, (((0,), (0,)), ((), ())), preferred_element_type=jnp.float32
    )


def head_norm(x, gain):
    r = lax.rsqrt(jnp.mean(x * x, axis=-1, keepdims=True) + epsilon)
    return r, (x * r * gain).astype(jnp.bfloat16)


def norm_backward(x, r, gain, upstream):
    w = upstream * gain
    inner = jnp.mean(w * x, axis=-1, keepdims=True)
    return r * w - x * (r * r * r) * inner


def block_count(length):
    return (length + (ROW_SLOTS - 1)) // ROW_SLOTS


def folded(x):
    return jnp.sum(x.reshape(-1, 8, x.shape[-1]), axis=0)


def causal(keys, rows, first):
    slot = lax.broadcasted_iota(jnp.int32, (keys, rows), 1) & (ROW_SLOTS - 1)
    return lax.broadcasted_iota(jnp.int32, (keys, rows), 0) <= slot + first


def exponent(k, q):
    return jnp.exp2(contract_last(k, q) * (k.shape[-1] ** (-0.5) * LOG2_E))


def before_kernel(
    meta, q_own, g_own, k_own, v_own, q_other, g_other, k_other, v_other, q_gain, k_gain,
    qs, gs, partial,
):
    slots, width = q_own.shape
    head_dim = k_own.shape[1]
    group = width // head_dim
    rows = ROW_SLOTS * group
    gain_q, gain_k = q_gain[...], k_gain[...]
    units = ((q_own, g_own, k_own, v_own), (q_other, g_other, k_other, v_other))
    for which, (q_ref, g_ref, k_ref, v_ref) in enumerate(units):
        length = meta[2 * which]
        _, kn = head_norm(k_ref[...].astype(jnp.float32), gain_k)

        def row_block(b, carry, which=which, q_ref=q_ref, g_ref=g_ref, v_ref=v_ref, kn=kn, length=length):
            first = pl.multiple_of(b * ROW_SLOTS, ROW_SLOTS)
            at = pl.ds(first, ROW_SLOTS)
            out = pl.multiple_of(b * rows, rows)
            live = lax.broadcasted_iota(jnp.int32, (ROW_SLOTS, head_dim), 0) + first < length
            normed, grads = [], []
            for g in range(group):
                cols = slice(g * head_dim, (g + 1) * head_dim)
                normed.append(head_norm(q_ref[at, cols].astype(jnp.float32), gain_q)[1])
                grad = g_ref[at, cols].astype(jnp.float32)
                grads.append(jnp.where(live, grad, 0.0).astype(jnp.bfloat16))
            q, go = jnp.concatenate(normed, axis=0), jnp.concatenate(grads, axis=0)
            qs[0, which, pl.ds(out, rows), :] = q
            gs[0, which, pl.ds(out, rows), :] = go
            e = jnp.where(causal(slots, rows, first), exponent(kn, q), 0.0)
            stats = pl.multiple_of(b * 16, 16)
            partial[0, which, pl.ds(stats, 8), :] = folded(e)
            partial[0, which, pl.ds(stats + 8, 8), :] = folded(e * contract_last(v_ref[...], go))
            return carry

        lax.fori_loop(0, block_count(length), row_block, 0)


def prompt_kernel(
    meta, prompt, qs, gs, partial, ds_out, stats, prompt_grads,
    e_0, dp_0, e_1, dp_1, dk_acc, dv_acc,
):
    total = prompt.shape[0]
    head_dim = qs.shape[-1]
    rows = e_0.shape[1]
    buffers = ((e_0, dp_0), (e_1, dp_1))
    which = pl.program_id(1)
    length, seen = meta[2 * which], meta[2 * which + 1]

    @pl.when(which == 0)
    def _():
        dk_acc[...] = jnp.zeros(dk_acc.shape, jnp.float32)
        dv_acc[...] = jnp.zeros(dv_acc.shape, jnp.float32)

    def first_pass(low, high, b, e_s, dp_s):
        at = pl.ds(pl.multiple_of(b * rows, rows), rows)
        q, go = qs[0, 0, at, :], gs[0, 0, at, :]
        part = pl.multiple_of(b * 16, 16)
        sums = partial[0, 0, pl.ds(part, 8), :]
        dots = partial[0, 0, pl.ds(part + 8, 8), :]
        for base in range(0, high, KEY_CHUNK):
            chunk = slice(base, base + KEY_CHUNK)
            e = exponent(prompt[chunk, :head_dim], q)
            if base + KEY_CHUNK > low:
                index = lax.broadcasted_iota(jnp.int32, (KEY_CHUNK, rows), 0)
                e = jnp.where(index < seen - base, e, 0.0)
            dp = contract_last(prompt[chunk, head_dim:], go)
            e_s[chunk] = e
            dp_s[chunk] = dp
            sums += folded(e)
            dots += folded(e * dp)
        inverse = 1.0 / jnp.sum(sums, axis=0, keepdims=True)
        delta = jnp.sum(dots, axis=0, keepdims=True) * inverse
        stats[0, 0, pl.ds(part, 8), :] = jnp.broadcast_to(inverse, (8, rows))
        stats[0, 0, pl.ds(part + 8, 8), :] = jnp.broadcast_to(delta, (8, rows))
        return q, go, inverse, delta

    def second_pass(high, b, e_s, dp_s, q, go, inverse, delta):
        for base in range(0, high, KEY_CHUNK):
            chunk = slice(base, base + KEY_CHUNK)
            p = e_s[chunk] * inverse
            ds = (p * (dp_s[chunk] - delta)).astype(jnp.bfloat16)
            ds_out[0, 0, b, chunk, :] = ds
            dv_acc[chunk] += jnp.dot(
                p.astype(jnp.bfloat16), go, preferred_element_type=jnp.float32
            )
            dk_acc[chunk] += jnp.dot(ds, q, preferred_element_type=jnp.float32)

    def blocks(low, high):
        def run(some):
            held = [first_pass(low, high, b, *buffers[i]) for i, b in enumerate(some)]
            for i, b in enumerate(some):
                second_pass(high, b, *buffers[i], *held[i])

        def pair(i, carry):
            run((2 * i, 2 * i + 1))
            return carry

        count = block_count(length)
        lax.fori_loop(0, count // 2, pair, 0)

        @pl.when(count % 2 == 1)
        def _():
            run((count - 1,))

    step = total // KEY_STEPS
    for n in range(1, KEY_STEPS + 1):
        low, high = (n - 1) * step, n * step
        pl.when((seen > low) & (seen <= high))(functools.partial(blocks, low, high))

    @pl.when(which == pl.num_programs(1) - 1)
    def _():
        scale = head_dim ** (-0.5)
        prompt_grads[:, :head_dim] = (dk_acc[...] * scale).astype(jnp.bfloat16)
        prompt_grads[:, head_dim:] = dv_acc[...].astype(jnp.bfloat16)


def after_kernel(
    meta, q_own, k_own, v_own, q_other, k_other, v_other, prompt, qs, gs, ds_in, stats,
    q_gain, k_gain,
    dq_own, dk_own, dv_own, dq_other, dk_other, dv_other, dk_acc, dv_acc,
):
    slots, width = q_own.shape
    head_dim = k_own.shape[1]
    group = width // head_dim
    rows = ROW_SLOTS * group
    total = prompt.shape[0]
    scale = head_dim ** (-0.5)
    gain_q, gain_k = q_gain[...], k_gain[...]
    units = (
        (q_own, k_own, v_own, dq_own, dk_own, dv_own),
        (q_other, k_other, v_other, dq_other, dk_other, dv_other),
    )
    for which, (q_ref, k_ref, v_ref, dq_ref, dk_ref, dv_ref) in enumerate(units):
        length, seen = meta[2 * which], meta[2 * which + 1]
        key_x = k_ref[...].astype(jnp.float32)
        key_r, kn = head_norm(key_x, gain_k)
        dq_ref[...] = jnp.zeros(dq_ref.shape, dq_ref.dtype)
        dk_acc[...] = jnp.zeros(dk_acc.shape, jnp.float32)
        dv_acc[...] = jnp.zeros(dv_acc.shape, jnp.float32)

        def blocks(high, which=which, q_ref=q_ref, v_ref=v_ref, dq_ref=dq_ref, kn=kn, length=length):
            def row_block(b, carry):
                first = pl.multiple_of(b * ROW_SLOTS, ROW_SLOTS)
                at = pl.ds(pl.multiple_of(b * rows, rows), rows)
                q, go = qs[0, which, at, :], gs[0, which, at, :]
                part = pl.multiple_of(b * 16, 16)
                inverse = stats[0, which, pl.ds(part, 8), :][:1]
                delta = stats[0, which, pl.ds(part + 8, 8), :][:1]
                e = jnp.where(causal(slots, rows, first), exponent(kn, q), 0.0)
                p = e * inverse
                ds = (p * (contract_last(v_ref[...], go) - delta)).astype(jnp.bfloat16)
                dv_acc[...] += jnp.dot(
                    p.astype(jnp.bfloat16), go, preferred_element_type=jnp.float32
                )
                dk_acc[...] += jnp.dot(ds, q, preferred_element_type=jnp.float32)
                dq = contract_first(ds, kn) + contract_first(
                    ds_in[0, which, b, :high, :], prompt[:high, :head_dim]
                )
                dq = dq * scale
                for g in range(group):
                    cols = slice(g * head_dim, (g + 1) * head_dim)
                    x = q_ref[pl.ds(first, ROW_SLOTS), cols].astype(jnp.float32)
                    r = lax.rsqrt(jnp.mean(x * x, axis=-1, keepdims=True) + epsilon)
                    up = dq[g * ROW_SLOTS : (g + 1) * ROW_SLOTS]
                    dx = norm_backward(x, r, gain_q, up)
                    dq_ref[pl.ds(first, ROW_SLOTS), cols] = dx.astype(jnp.bfloat16)
                return carry

            lax.fori_loop(0, block_count(length), row_block, 0)

        step = total // KEY_STEPS
        for n in range(1, KEY_STEPS + 1):
            low, high = (n - 1) * step, n * step
            pl.when((seen > low) & (seen <= high))(functools.partial(blocks, high))
        dk = norm_backward(key_x, key_r, gain_k, dk_acc[...] * scale)
        dk_ref[...] = dk.astype(jnp.bfloat16)
        dv_ref[...] = dv_acc[...].astype(jnp.bfloat16)


def attend(heads, meta, own, other, prompt, weight_pair, q_gain, k_gain, width, head_dim):
    slots, total = own.shape[0], prompt.shape[0]
    group = width // head_dim
    rows = ROW_SLOTS * group
    steps = slots // ROW_SLOTS
    narrow = 2 * heads * group
    low, high = jnp.bfloat16, jnp.float32
    scalars = pl.BlockSpec(memory_space=pltpu.SMEM)
    gain = pl.BlockSpec((1, head_dim), lambda *i: (0, 0))

    def columns(block, index):
        return pl.BlockSpec((slots, block), lambda i, index=index: (0, index + i))

    def by_head(rows, block):
        return pl.BlockSpec((rows, block), lambda i, *_: (0, i))

    def by_pair(*shape):
        return pl.BlockSpec((1, 2, *shape), lambda i: (i, 0) + (0,) * len(shape))

    def by_unit(*shape):
        return pl.BlockSpec((1, 1, *shape), lambda i, k: (i, k) + (0,) * len(shape))

    def cost(products, keys, moved):
        return pl.CostEstimate(
            flops=heads * 2 * products * 2 * slots * group * keys * head_dim,
            bytes_accessed=moved,
            transcendentals=heads * 2 * slots * group * keys,
        )

    q_side = columns(width, 0)
    g_side = columns(width, heads)
    k_side = columns(head_dim, narrow)
    v_side = columns(head_dim, narrow + heads)
    stack, stat, shade = (steps * rows, head_dim), (steps * 16, rows), (steps, total, rows)

    def limit(mebibytes):
        return pltpu.CompilerParams(vmem_limit_bytes=mebibytes * 1024 * 1024)

    def shaped(shape, kind):
        return jax.ShapeDtypeStruct((heads, 2, *shape), kind)

    qs, gs, partial = pl.pallas_call(
        before_kernel,
        grid=(heads,),
        in_specs=[scalars, q_side, g_side, k_side, v_side, q_side, g_side, k_side, v_side, gain, gain],
        out_specs=[by_pair(*stack), by_pair(*stack), by_pair(*stat)],
        out_shape=[shaped(stack, low), shaped(stack, low), shaped(stat, high)],
        compiler_params=limit(8),
        cost_estimate=cost(2, slots, 4 * 1024 * 1024),
    )(meta, own, own, own, own, other, other, other, other, q_gain, k_gain)
    above = [shifted(weight_pair, -k) for k in (1, 2, 3)]
    above.append(shifted(above[-1], -1))
    weight_pair, prompt, qs, gs, partial, *above = lax.optimization_barrier(
        (weight_pair, prompt, qs, gs, partial, *above)
    )
    below = []
    for k in (3, 2, 1):
        below.append(shifted(weight_pair, k))
    middle = pl.pallas_call(
        prompt_kernel,
        grid=(heads, 2),
        in_specs=[scalars, by_head(total, 2 * head_dim), by_unit(*stack), by_unit(*stack), by_unit(*stat)],
        out_specs=[by_unit(*shade), by_unit(*stat), by_head(total, 2 * head_dim)],
        out_shape=[
            shaped(shade, low),
            shaped(stat, high),
            jax.ShapeDtypeStruct((total, heads * 2 * head_dim), low),
        ],
        scratch_shapes=[
            pltpu.VMEM((total, rows), high),
            pltpu.VMEM((total, rows), high),
            pltpu.VMEM((total, rows), high),
            pltpu.VMEM((total, rows), high),
            pltpu.VMEM((total, head_dim), high),
            pltpu.VMEM((total, head_dim), high),
        ],
        compiler_params=limit(57),
        cost_estimate=cost(4, total, 12 * 1024 * 1024),
    )
    ds, stats, prompt_grads = middle(meta, prompt, qs, gs, partial)
    outs = [(slots, width), (slots, head_dim), (slots, head_dim)] * 2
    last = pl.pallas_call(
        after_kernel,
        grid=(heads,),
        in_specs=[scalars, q_side, k_side, v_side, q_side, k_side, v_side]
        + [by_head(total, 2 * head_dim), by_pair(*stack), by_pair(*stack)]
        + [by_pair(*shade), by_pair(*stat), gain, gain],
        out_specs=[by_head(*s) for s in outs],
        out_shape=[jax.ShapeDtypeStruct((n, heads * m), low) for n, m in outs],
        scratch_shapes=[pltpu.VMEM((slots, head_dim), high), pltpu.VMEM((slots, head_dim), high)],
        compiler_params=limit(57),
        cost_estimate=cost(2, total, 14 * 1024 * 1024),
    )
    grads = last(
        meta, own, own, own, other, other, other, prompt, qs, gs, ds, stats, q_gain, k_gain
    )
    return (*grads, prompt_grads, [weight_pair, *above, *below])


def on_device(
    prompt_key_rows,
    prompt_value_rows,
    queries,
    keys,
    values,
    output_gradient,
    lengths,
    prompt_visible_rows,
    query_gain,
    key_norm_gain,
    key_value_weight,
):
    head_dim = query_gain.shape[0]
    core = lax.axis_index(PAIR)
    cores = lax.axis_size(PAIR)
    heads = keys.shape[1] // head_dim // cores
    narrow = heads * head_dim
    wide = queries.shape[1] // cores
    width = wide // heads
    near, far = lax.axis_size(NEAR), lax.axis_size(FAR)
    q_gain, k_gain = query_gain[None, :], key_norm_gain[None, :]

    def part(a, which, n):
        return lax.dynamic_slice_in_dim(a, which * n, n, axis=1)

    def in_core_order(mine, theirs):
        flip = core == 0
        return jnp.where(flip, mine, theirs), jnp.where(flip, theirs, mine)

    def prompt_part(which):
        return jnp.concatenate(
            [part(prompt_key_rows, which, narrow), part(prompt_value_rows, which, narrow)], axis=1
        )

    def pack(which):
        return jnp.concatenate(
            [
                part(queries, which, wide),
                part(output_gradient, which, wide),
                part(keys, which, narrow),
                part(values, which, narrow),
            ],
            axis=1,
        )

    def weight_part(which):
        cut = key_value_weight.reshape(-1, 2, cores, heads, head_dim)
        cut = lax.dynamic_index_in_dim(cut, which, 2, keepdims=False)
        return cut.transpose(0, 2, 1, 3).reshape(-1, 2 * narrow)

    raw = jnp.concatenate(in_core_order(prompt_part(core), swap(prompt_part(1 - core))), axis=0)
    count = raw.shape[0]
    px = raw[:, :narrow].astype(jnp.float32).reshape(count, heads, head_dim)
    pr = lax.rsqrt(jnp.mean(px * px, axis=-1, keepdims=True) + epsilon)
    pn = (px * pr * key_norm_gain).astype(jnp.bfloat16).reshape(count, narrow)
    pv = raw[:, narrow:]

    meta_own = jnp.stack([lengths[0], prompt_visible_rows[0]])
    meta = jnp.concatenate([meta_own, swap(meta_own)])
    own, other = pack(core), swap(pack(1 - core))
    weight_pair = jnp.concatenate(
        in_core_order(weight_part(core), swap(weight_part(1 - core))), axis=0
    )

    both = jnp.concatenate(
        [
            a[:, h * head_dim : (h + 1) * head_dim]
            for h in range(heads)
            for a in (pn, pv)
        ],
        axis=1,
    )
    prompt = from_everyone(both, PLANE).reshape(-1, 2 * narrow)

    results = attend(
        heads, meta, own, other, prompt, weight_pair, q_gain, k_gain, width, head_dim
    )

    sent, *rows_from = lax.optimization_barrier((results[6], *results[7]))
    ring = jnp.stack(rows_from + rows_from)
    weight = lax.dynamic_slice_in_dim(ring, far - lax.axis_index(FAR), far, axis=0)
    weight = weight.reshape(-1, 2 * narrow)
    sent = sent.reshape(far * near, count, 2 * narrow)
    parts = lax.all_to_all(sent, PLANE, 0, 0, tiled=True)
    total = jnp.sum(parts.astype(jnp.float32), axis=0).reshape(count, heads, 2, head_dim)
    w = total[:, :, 0] * key_norm_gain
    inner = jnp.mean(w * px, axis=-1, keepdims=True)
    dk = pr * w - px * (pr * pr * pr) * inner
    grads = jnp.stack([dk, total[:, :, 1]], axis=2).reshape(count, 2 * narrow)
    rows = from_everyone(grads.astype(jnp.bfloat16), NEAR).reshape(-1, 2 * narrow)

    def assembled(index):
        return jnp.concatenate(in_core_order(results[index], swap(results[index + 3])), axis=1)

    query_grad, key_grad, value_grad = assembled(0), assembled(1), assembled(2)

    hidden = contract_last(rows, weight)
    per_core = count // cores
    hidden = hidden.reshape(near, cores, per_core, -1)
    mine = lax.dynamic_index_in_dim(hidden, core, 1, keepdims=False)
    theirs = lax.dynamic_index_in_dim(hidden, 1 - core, 1, keepdims=False)
    mine = (mine + swap(theirs.astype(jnp.bfloat16)).astype(jnp.float32)).astype(jnp.bfloat16)
    arrived = lax.all_to_all(mine, NEAR, 0, 0, tiled=True)
    arrived = arrived.reshape(near, per_core, far, -1)
    hidden_grad = arrived.transpose(1, 2, 0, 3).reshape(per_core, -1)
    return (query_grad, key_grad, value_grad, hidden_grad)


def solution(mesh):
    finer = Mesh(
        mesh.devices.reshape(mesh.shape["grp"], 8, 8, 2), ("grp", "cand_0", "cand_1", "cand_2")
    )
    return jax.shard_map(
        on_device,
        mesh=finer,
        in_specs=(
            P(GRP_CAND, None),
            P(GRP_CAND, None),
            P(GRP_CAND, None),
            P(GRP_CAND, None),
            P(GRP_CAND, None),
            P(GRP_CAND, None),
            P(GRP_CAND),
            P(GRP_CAND),
            P(),
            P(),
            P(CAND, None),
        ),
        out_specs=(P(GRP_CAND, None), P(GRP_CAND, None), P(GRP_CAND, None), P(GRP_CAND, None)),
        check_vma=False,
    )
```

```python
import functools

import jax
import jax.numpy as jnp
from jax import lax
from jax.experimental import pallas as pl
from jax.experimental.pallas import tpu as pltpu
from jax.sharding import Mesh
from jax.sharding import PartitionSpec as P


CAND = ("cand_0", "cand_1", "cand_2")
GRP_CAND = ("grp", "cand_0", "cand_1", "cand_2")
PLANE = ("cand_0", "cand_1")
FAR, NEAR, PAIR = CAND
NEARBY = (3, 2, 1)
ROW_SLOTS = 32
KEY_CHUNK = 128
KEY_STEPS = 4
LOG2_E = 1.4426950408889634

epsilon = 1e-06


def swap(x):
    return lax.ppermute(x, PAIR, [(0, 1), (1, 0)])


def shifted(x, by):
    n = lax.axis_size(FAR)
    return lax.ppermute(x, FAR, [(i, (i + by) % n) for i in range(n)])


def from_everyone(shard, axis):
    copies = jnp.broadcast_to(shard, (lax.axis_size(axis), *shard.shape))
    return lax.all_to_all(copies, axis, split_axis=0, concat_axis=0, tiled=True)


def contract_last(left, right):
    return lax.dot_general(
        left, right, (((1,), (1,)), ((), ())), preferred_element_type=jnp.float32
    )


def contract_first(left, right):
    return lax.dot_general(
        left, right, (((0,), (0,)), ((), ())), preferred_element_type=jnp.float32
    )


def head_norm(x, gain):
    r = lax.rsqrt(jnp.mean(x * x, axis=-1, keepdims=True) + epsilon)
    return r, (x * r * gain).astype(jnp.bfloat16)


def norm_backward(x, r, gain, upstream):
    w = upstream * gain
    inner = jnp.mean(w * x, axis=-1, keepdims=True)
    return r * w - x * (r * r * r) * inner


def block_count(length):
    return (length + (ROW_SLOTS - 1)) // ROW_SLOTS


def folded(x):
    return jnp.sum(x.reshape(-1, 8, x.shape[-1]), axis=0)


def causal(keys, rows, first):
    slot = lax.broadcasted_iota(jnp.int32, (keys, rows), 1) & (ROW_SLOTS - 1)
    return lax.broadcasted_iota(jnp.int32, (keys, rows), 0) <= slot + first


def exponent(k, q):
    return jnp.exp2(contract_last(k, q) * (k.shape[-1] ** (-0.5) * LOG2_E))


def before_kernel(
    meta, q_own, g_own, k_own, v_own, q_other, g_other, k_other, v_other, q_gain, k_gain,
    qs, gs, partial,
):
    slots, width = q_own.shape
    head_dim = k_own.shape[1]
    group = width // head_dim
    rows = ROW_SLOTS * group
    gain_q, gain_k = q_gain[...], k_gain[...]
    units = ((q_own, g_own, k_own, v_own), (q_other, g_other, k_other, v_other))
    for which, (q_ref, g_ref, k_ref, v_ref) in enumerate(units):
        length = meta[2 * which]
        _, kn = head_norm(k_ref[...].astype(jnp.float32), gain_k)

        def row_block(b, carry, which=which, q_ref=q_ref, g_ref=g_ref, v_ref=v_ref, kn=kn, length=length):
            first = pl.multiple_of(b * ROW_SLOTS, ROW_SLOTS)
            at = pl.ds(first, ROW_SLOTS)
            out = pl.multiple_of(b * rows, rows)
            live = lax.broadcasted_iota(jnp.int32, (ROW_SLOTS, head_dim), 0) + first < length
            normed, grads = [], []
            for g in range(group):
                cols = slice(g * head_dim, (g + 1) * head_dim)
                normed.append(head_norm(q_ref[at, cols].astype(jnp.float32), gain_q)[1])
                grad = g_ref[at, cols].astype(jnp.float32)
                grads.append(jnp.where(live, grad, 0.0).astype(jnp.bfloat16))
            q, go = jnp.concatenate(normed, axis=0), jnp.concatenate(grads, axis=0)
            qs[0, which, pl.ds(out, rows), :] = q
            gs[0, which, pl.ds(out, rows), :] = go
            e = jnp.where(causal(slots, rows, first), exponent(kn, q), 0.0)
            stats = pl.multiple_of(b * 16, 16)
            partial[0, which, pl.ds(stats, 8), :] = folded(e)
            partial[0, which, pl.ds(stats + 8, 8), :] = folded(e * contract_last(v_ref[...], go))
            return carry

        lax.fori_loop(0, block_count(length), row_block, 0)


def prompt_kernel(
    meta, prompt, qs, gs, partial, ds_out, stats, prompt_grads,
    e_0, dp_0, e_1, dp_1, dk_acc, dv_acc,
):
    total = prompt.shape[0]
    head_dim = qs.shape[-1]
    rows = e_0.shape[1]
    buffers = ((e_0, dp_0), (e_1, dp_1))
    which = pl.program_id(1)
    length, seen = meta[2 * which], meta[2 * which + 1]

    @pl.when(which == 0)
    def _():
        dk_acc[...] = jnp.zeros(dk_acc.shape, jnp.float32)
        dv_acc[...] = jnp.zeros(dv_acc.shape, jnp.float32)

    def first_pass(low, high, b, e_s, dp_s):
        at = pl.ds(pl.multiple_of(b * rows, rows), rows)
        q, go = qs[0, 0, at, :], gs[0, 0, at, :]
        part = pl.multiple_of(b * 16, 16)
        sums = partial[0, 0, pl.ds(part, 8), :]
        dots = partial[0, 0, pl.ds(part + 8, 8), :]
        for base in range(0, high, KEY_CHUNK):
            chunk = slice(base, base + KEY_CHUNK)
            e = exponent(prompt[chunk, :head_dim], q)
            if base + KEY_CHUNK > low:
                index = lax.broadcasted_iota(jnp.int32, (KEY_CHUNK, rows), 0)
                e = jnp.where(index < seen - base, e, 0.0)
            dp = contract_last(prompt[chunk, head_dim:], go)
            e_s[chunk] = e
            dp_s[chunk] = dp
            sums += folded(e)
            dots += folded(e * dp)
        inverse = 1.0 / jnp.sum(sums, axis=0, keepdims=True)
        delta = jnp.sum(dots, axis=0, keepdims=True) * inverse
        stats[0, 0, pl.ds(part, 8), :] = jnp.broadcast_to(inverse, (8, rows))
        stats[0, 0, pl.ds(part + 8, 8), :] = jnp.broadcast_to(delta, (8, rows))
        return q, go, inverse, delta

    def second_pass(high, b, e_s, dp_s, q, go, inverse, delta):
        for base in range(0, high, KEY_CHUNK):
            chunk = slice(base, base + KEY_CHUNK)
            p = e_s[chunk] * inverse
            ds = (p * (dp_s[chunk] - delta)).astype(jnp.bfloat16)
            ds_out[0, 0, b, chunk, :] = ds
            dv_acc[chunk] += jnp.dot(
                p.astype(jnp.bfloat16), go, preferred_element_type=jnp.float32
            )
            dk_acc[chunk] += jnp.dot(ds, q, preferred_element_type=jnp.float32)

    def blocks(low, high):
        def run(some):
            held = [first_pass(low, high, b, *buffers[i]) for i, b in enumerate(some)]
            for i, b in enumerate(some):
                second_pass(high, b, *buffers[i], *held[i])

        def pair(i, carry):
            run((2 * i, 2 * i + 1))
            return carry

        count = block_count(length)
        lax.fori_loop(0, count // 2, pair, 0)

        @pl.when(count % 2 == 1)
        def _():
            run((count - 1,))

    step = total // KEY_STEPS
    for n in range(1, KEY_STEPS + 1):
        low, high = (n - 1) * step, n * step
        pl.when((seen > low) & (seen <= high))(functools.partial(blocks, low, high))

    @pl.when(which == pl.num_programs(1) - 1)
    def _():
        scale = head_dim ** (-0.5)
        prompt_grads[:, :head_dim] = (dk_acc[...] * scale).astype(jnp.bfloat16)
        prompt_grads[:, head_dim:] = dv_acc[...].astype(jnp.bfloat16)


def after_kernel(
    meta, q_own, k_own, v_own, q_other, k_other, v_other, prompt, qs, gs, ds_in, stats,
    q_gain, k_gain,
    dq_own, dk_own, dv_own, dq_other, dk_other, dv_other, dk_acc, dv_acc,
):
    slots, width = q_own.shape
    head_dim = k_own.shape[1]
    group = width // head_dim
    rows = ROW_SLOTS * group
    total = prompt.shape[0]
    scale = head_dim ** (-0.5)
    gain_q, gain_k = q_gain[...], k_gain[...]
    units = (
        (q_own, k_own, v_own, dq_own, dk_own, dv_own),
        (q_other, k_other, v_other, dq_other, dk_other, dv_other),
    )
    for which, (q_ref, k_ref, v_ref, dq_ref, dk_ref, dv_ref) in enumerate(units):
        length, seen = meta[2 * which], meta[2 * which + 1]
        key_x = k_ref[...].astype(jnp.float32)
        key_r, kn = head_norm(key_x, gain_k)
        dq_ref[...] = jnp.zeros(dq_ref.shape, dq_ref.dtype)
        dk_acc[...] = jnp.zeros(dk_acc.shape, jnp.float32)
        dv_acc[...] = jnp.zeros(dv_acc.shape, jnp.float32)

        def blocks(high, which=which, q_ref=q_ref, v_ref=v_ref, dq_ref=dq_ref, kn=kn, length=length):
            def row_block(b, carry):
                first = pl.multiple_of(b * ROW_SLOTS, ROW_SLOTS)
                at = pl.ds(pl.multiple_of(b * rows, rows), rows)
                q, go = qs[0, which, at, :], gs[0, which, at, :]
                part = pl.multiple_of(b * 16, 16)
                inverse = stats[0, which, pl.ds(part, 8), :][:1]
                delta = stats[0, which, pl.ds(part + 8, 8), :][:1]
                e = jnp.where(causal(slots, rows, first), exponent(kn, q), 0.0)
                p = e * inverse
                ds = (p * (contract_last(v_ref[...], go) - delta)).astype(jnp.bfloat16)
                dv_acc[...] += jnp.dot(
                    p.astype(jnp.bfloat16), go, preferred_element_type=jnp.float32
                )
                dk_acc[...] += jnp.dot(ds, q, preferred_element_type=jnp.float32)
                dq = contract_first(ds, kn) + contract_first(
                    ds_in[0, which, b, :high, :], prompt[:high, :head_dim]
                )
                dq = dq * scale
                for g in range(group):
                    cols = slice(g * head_dim, (g + 1) * head_dim)
                    x = q_ref[pl.ds(first, ROW_SLOTS), cols].astype(jnp.float32)
                    r = lax.rsqrt(jnp.mean(x * x, axis=-1, keepdims=True) + epsilon)
                    up = dq[g * ROW_SLOTS : (g + 1) * ROW_SLOTS]
                    dx = norm_backward(x, r, gain_q, up)
                    dq_ref[pl.ds(first, ROW_SLOTS), cols] = dx.astype(jnp.bfloat16)
                return carry

            lax.fori_loop(0, block_count(length), row_block, 0)

        step = total // KEY_STEPS
        for n in range(1, KEY_STEPS + 1):
            low, high = (n - 1) * step, n * step
            pl.when((seen > low) & (seen <= high))(functools.partial(blocks, high))
        dk = norm_backward(key_x, key_r, gain_k, dk_acc[...] * scale)
        dk_ref[...] = dk.astype(jnp.bfloat16)
        dv_ref[...] = dv_acc[...].astype(jnp.bfloat16)


def place_kernel(place, *refs):
    blocks, out = refs[:-1], refs[-1]
    for j, block in enumerate(blocks):
        out[lax.rem(place[0] + j, len(blocks))] = block[...]


def attend(heads, meta, own, other, prompt, weight_pair, q_gain, k_gain, width, head_dim):
    slots, total = own.shape[0], prompt.shape[0]
    group = width // head_dim
    rows = ROW_SLOTS * group
    steps = slots // ROW_SLOTS
    narrow = 2 * heads * group
    low, high = jnp.bfloat16, jnp.float32
    scalars = pl.BlockSpec(memory_space=pltpu.SMEM)
    gain = pl.BlockSpec((1, head_dim), lambda *i: (0, 0))

    def columns(block, index):
        return pl.BlockSpec((slots, block), lambda i, index=index: (0, index + i))

    def by_head(rows, block):
        return pl.BlockSpec((rows, block), lambda i, *_: (0, i))

    def by_pair(*shape):
        return pl.BlockSpec((1, 2, *shape), lambda i: (i, 0) + (0,) * len(shape))

    def by_unit(*shape):
        return pl.BlockSpec((1, 1, *shape), lambda i, k: (i, k) + (0,) * len(shape))

    def cost(products, keys, moved):
        return pl.CostEstimate(
            flops=heads * 2 * products * 2 * slots * group * keys * head_dim,
            bytes_accessed=moved,
            transcendentals=heads * 2 * slots * group * keys,
        )

    q_side = columns(width, 0)
    g_side = columns(width, heads)
    k_side = columns(head_dim, narrow)
    v_side = columns(head_dim, narrow + heads)
    stack, stat, shade = (steps * rows, head_dim), (steps * 16, rows), (steps, total, rows)

    def limit(mebibytes):
        return pltpu.CompilerParams(vmem_limit_bytes=mebibytes * 1024 * 1024)

    def shaped(shape, kind):
        return jax.ShapeDtypeStruct((heads, 2, *shape), kind)

    qs, gs, partial = pl.pallas_call(
        before_kernel,
        grid=(heads,),
        in_specs=[scalars, q_side, g_side, k_side, v_side, q_side, g_side, k_side, v_side, gain, gain],
        out_specs=[by_pair(*stack), by_pair(*stack), by_pair(*stat)],
        out_shape=[shaped(stack, low), shaped(stack, low), shaped(stat, high)],
        compiler_params=limit(8),
        cost_estimate=cost(2, slots, 4 * 1024 * 1024),
    )(meta, own, own, own, own, other, other, other, other, q_gain, k_gain)
    weight_pair, prompt, qs, gs, partial = lax.optimization_barrier(
        (weight_pair, prompt, qs, gs, partial)
    )
    above, below = [], []
    for k in NEARBY:
        below.append(shifted(weight_pair, k))
        above.append(shifted(weight_pair, -k))
    middle = pl.pallas_call(
        prompt_kernel,
        grid=(heads, 2),
        in_specs=[scalars, by_head(total, 2 * head_dim), by_unit(*stack), by_unit(*stack), by_unit(*stat)],
        out_specs=[by_unit(*shade), by_unit(*stat), by_head(total, 2 * head_dim)],
        out_shape=[
            shaped(shade, low),
            shaped(stat, high),
            jax.ShapeDtypeStruct((total, heads * 2 * head_dim), low),
        ],
        scratch_shapes=[
            pltpu.VMEM((total, rows), high),
            pltpu.VMEM((total, rows), high),
            pltpu.VMEM((total, rows), high),
            pltpu.VMEM((total, rows), high),
            pltpu.VMEM((total, head_dim), high),
            pltpu.VMEM((total, head_dim), high),
        ],
        compiler_params=limit(57),
        cost_estimate=cost(4, total, 12 * 1024 * 1024),
    )
    ds, stats, prompt_grads = middle(meta, prompt, qs, gs, partial)
    outs = [(slots, width), (slots, head_dim), (slots, head_dim)] * 2
    last = pl.pallas_call(
        after_kernel,
        grid=(heads,),
        in_specs=[scalars, q_side, k_side, v_side, q_side, k_side, v_side]
        + [by_head(total, 2 * head_dim), by_pair(*stack), by_pair(*stack)]
        + [by_pair(*shade), by_pair(*stat), gain, gain],
        out_specs=[by_head(*s) for s in outs],
        out_shape=[jax.ShapeDtypeStruct((n, heads * m), low) for n, m in outs],
        scratch_shapes=[pltpu.VMEM((slots, head_dim), high), pltpu.VMEM((slots, head_dim), high)],
        compiler_params=limit(57),
        cost_estimate=cost(2, total, 14 * 1024 * 1024),
    )
    grads = last(
        meta, own, own, own, other, other, other, prompt, qs, gs, ds, stats, q_gain, k_gain
    )
    return (*grads, prompt_grads, [weight_pair, *above, *below])


def on_device(
    prompt_key_rows,
    prompt_value_rows,
    queries,
    keys,
    values,
    output_gradient,
    lengths,
    prompt_visible_rows,
    query_gain,
    key_norm_gain,
    key_value_weight,
):
    head_dim = query_gain.shape[0]
    core = lax.axis_index(PAIR)
    cores = lax.axis_size(PAIR)
    heads = keys.shape[1] // head_dim // cores
    narrow = heads * head_dim
    wide = queries.shape[1] // cores
    width = wide // heads
    near, far = lax.axis_size(NEAR), lax.axis_size(FAR)
    q_gain, k_gain = query_gain[None, :], key_norm_gain[None, :]

    def part(a, which, n):
        return lax.dynamic_slice_in_dim(a, which * n, n, axis=1)

    def in_core_order(mine, theirs):
        flip = core == 0
        return jnp.where(flip, mine, theirs), jnp.where(flip, theirs, mine)

    def prompt_part(which):
        return jnp.concatenate(
            [part(prompt_key_rows, which, narrow), part(prompt_value_rows, which, narrow)], axis=1
        )

    def pack(which):
        return jnp.concatenate(
            [
                part(queries, which, wide),
                part(output_gradient, which, wide),
                part(keys, which, narrow),
                part(values, which, narrow),
            ],
            axis=1,
        )

    def weight_part(which):
        cut = key_value_weight.reshape(-1, 2, cores, heads, head_dim)
        cut = lax.dynamic_index_in_dim(cut, which, 2, keepdims=False)
        return cut.transpose(0, 2, 1, 3).reshape(-1, 2 * narrow)

    raw = jnp.concatenate(in_core_order(prompt_part(core), swap(prompt_part(1 - core))), axis=0)
    count = raw.shape[0]
    px = raw[:, :narrow].astype(jnp.float32).reshape(count, heads, head_dim)
    pr = lax.rsqrt(jnp.mean(px * px, axis=-1, keepdims=True) + epsilon)
    pn = (px * pr * key_norm_gain).astype(jnp.bfloat16).reshape(count, narrow)
    pv = raw[:, narrow:]

    meta_own = jnp.stack([lengths[0], prompt_visible_rows[0]])
    meta = jnp.concatenate([meta_own, swap(meta_own)])
    own, other = pack(core), swap(pack(1 - core))
    weight_pair = jnp.concatenate(
        in_core_order(weight_part(core), swap(weight_part(1 - core))), axis=0
    )

    both = jnp.concatenate(
        [
            a[:, h * head_dim : (h + 1) * head_dim]
            for h in range(heads)
            for a in (pn, pv)
        ],
        axis=1,
    )
    prompt = from_everyone(both, PLANE).reshape(-1, 2 * narrow)

    results = attend(
        heads, meta, own, other, prompt, weight_pair, q_gain, k_gain, width, head_dim
    )

    sent, here, *arrived = lax.optimization_barrier((results[6], *results[7]))
    above, below = dict(zip(NEARBY, arrived[: len(NEARBY)])), dict(zip(NEARBY, arrived[len(NEARBY) :]))
    across = shifted(above[3], -1)
    ring = [here, above[1], above[2], above[3], across, below[3], below[2], below[1]]
    place = jnp.reshape(lax.axis_index(FAR), (1,))
    weight = pl.pallas_call(
        place_kernel,
        in_specs=[pl.BlockSpec(memory_space=pltpu.SMEM)]
        + [pl.BlockSpec(memory_space=pltpu.VMEM)] * far,
        out_specs=pl.BlockSpec(memory_space=pltpu.VMEM),
        out_shape=jax.ShapeDtypeStruct((far, *here.shape), here.dtype),
        compiler_params=pltpu.CompilerParams(vmem_limit_bytes=8 * 1024 * 1024),
        cost_estimate=pl.CostEstimate(
            flops=10**8, bytes_accessed=2 * far * here.size * 2, transcendentals=0
        ),
    )(place.astype(jnp.int32), *ring)
    weight = weight.reshape(-1, 2 * narrow)
    sent = sent.reshape(far * near, count, 2 * narrow)
    parts = lax.all_to_all(sent, PLANE, 0, 0, tiled=True)
    total = jnp.sum(parts.astype(jnp.float32), axis=0).reshape(count, heads, 2, head_dim)
    w = total[:, :, 0] * key_norm_gain
    inner = jnp.mean(w * px, axis=-1, keepdims=True)
    dk = pr * w - px * (pr * pr * pr) * inner
    grads = jnp.stack([dk, total[:, :, 1]], axis=2).reshape(count, 2 * narrow)
    rows = from_everyone(grads.astype(jnp.bfloat16), NEAR).reshape(-1, 2 * narrow)

    def assembled(index):
        return jnp.concatenate(in_core_order(results[index], swap(results[index + 3])), axis=1)

    query_grad, key_grad, value_grad = assembled(0), assembled(1), assembled(2)

    hidden = contract_last(rows, weight)
    per_core = count // cores
    hidden = hidden.reshape(near, cores, per_core, -1)
    mine = lax.dynamic_index_in_dim(hidden, core, 1, keepdims=False)
    theirs = lax.dynamic_index_in_dim(hidden, 1 - core, 1, keepdims=False)
    mine = (mine + swap(theirs.astype(jnp.bfloat16)).astype(jnp.float32)).astype(jnp.bfloat16)
    arrived = lax.all_to_all(mine, NEAR, 0, 0, tiled=True)
    arrived = arrived.reshape(near, per_core, far, -1)
    hidden_grad = arrived.transpose(1, 2, 0, 3).reshape(per_core, -1)
    return (query_grad, key_grad, value_grad, hidden_grad)


def solution(mesh):
    finer = Mesh(
        mesh.devices.reshape(mesh.shape["grp"], 8, 8, 2), ("grp", "cand_0", "cand_1", "cand_2")
    )
    return jax.shard_map(
        on_device,
        mesh=finer,
        in_specs=(
            P(GRP_CAND, None),
            P(GRP_CAND, None),
            P(GRP_CAND, None),
            P(GRP_CAND, None),
            P(GRP_CAND, None),
            P(GRP_CAND, None),
            P(GRP_CAND),
            P(GRP_CAND),
            P(),
            P(),
            P(CAND, None),
        ),
        out_specs=(P(GRP_CAND, None), P(GRP_CAND, None), P(GRP_CAND, None), P(GRP_CAND, None)),
        check_vma=False,
    )
```

```python
import functools

import jax
import jax.numpy as jnp
from jax import lax
from jax.experimental import pallas as pl
from jax.experimental.pallas import tpu as pltpu
from jax.sharding import Mesh
from jax.sharding import PartitionSpec as P


CAND = ("cand_0", "cand_1", "cand_2")
GRP_CAND = ("grp", "cand_0", "cand_1", "cand_2")
PLANE = ("cand_0", "cand_1")
FAR, NEAR, PAIR = CAND
NEARBY = (3, 2, 1)
ROW_SLOTS = 32
KEY_CHUNK = 128
KEY_STEPS = 4
LOG2_E = 1.4426950408889634

epsilon = 1e-06


def swap(x):
    return lax.ppermute(x, PAIR, [(0, 1), (1, 0)])


def shifted(x, by):
    n = lax.axis_size(FAR)
    return lax.ppermute(x, FAR, [(i, (i + by) % n) for i in range(n)])


def from_everyone(shard, axis):
    copies = jnp.broadcast_to(shard, (lax.axis_size(axis), *shard.shape))
    return lax.all_to_all(copies, axis, split_axis=0, concat_axis=0, tiled=True)


def contract_last(left, right):
    return lax.dot_general(
        left, right, (((1,), (1,)), ((), ())), preferred_element_type=jnp.float32
    )


def contract_first(left, right):
    return lax.dot_general(
        left, right, (((0,), (0,)), ((), ())), preferred_element_type=jnp.float32
    )


def head_norm(x, gain):
    r = lax.rsqrt(jnp.mean(x * x, axis=-1, keepdims=True) + epsilon)
    return r, (x * r * gain).astype(jnp.bfloat16)


def norm_backward(x, r, gain, upstream):
    w = upstream * gain
    inner = jnp.mean(w * x, axis=-1, keepdims=True)
    return r * w - x * (r * r * r) * inner


def block_count(length):
    return (length + (ROW_SLOTS - 1)) // ROW_SLOTS


def folded(x):
    return jnp.sum(x.reshape(-1, 8, x.shape[-1]), axis=0)


def causal(keys, rows, first):
    slot = lax.broadcasted_iota(jnp.int32, (keys, rows), 1) & (ROW_SLOTS - 1)
    return lax.broadcasted_iota(jnp.int32, (keys, rows), 0) <= slot + first


def exponent(k, q):
    return jnp.exp2(contract_last(k, q) * (k.shape[-1] ** (-0.5) * LOG2_E))


def before_kernel(
    meta, q_own, g_own, k_own, v_own, q_other, g_other, k_other, v_other, q_gain, k_gain,
    qs, gs, partial,
):
    slots, width = q_own.shape
    head_dim = k_own.shape[1]
    group = width // head_dim
    rows = ROW_SLOTS * group
    gain_q, gain_k = q_gain[...], k_gain[...]
    units = ((q_own, g_own, k_own, v_own), (q_other, g_other, k_other, v_other))
    for which, (q_ref, g_ref, k_ref, v_ref) in enumerate(units):
        length = meta[2 * which]
        _, kn = head_norm(k_ref[...].astype(jnp.float32), gain_k)

        def row_block(b, carry, which=which, q_ref=q_ref, g_ref=g_ref, v_ref=v_ref, kn=kn, length=length):
            first = pl.multiple_of(b * ROW_SLOTS, ROW_SLOTS)
            at = pl.ds(first, ROW_SLOTS)
            out = pl.multiple_of(b * rows, rows)
            live = lax.broadcasted_iota(jnp.int32, (ROW_SLOTS, head_dim), 0) + first < length
            normed, grads = [], []
            for g in range(group):
                cols = slice(g * head_dim, (g + 1) * head_dim)
                normed.append(head_norm(q_ref[at, cols].astype(jnp.float32), gain_q)[1])
                grad = g_ref[at, cols].astype(jnp.float32)
                grads.append(jnp.where(live, grad, 0.0).astype(jnp.bfloat16))
            q, go = jnp.concatenate(normed, axis=0), jnp.concatenate(grads, axis=0)
            qs[0, which, pl.ds(out, rows), :] = q
            gs[0, which, pl.ds(out, rows), :] = go
            e = jnp.where(causal(slots, rows, first), exponent(kn, q), 0.0)
            stats = pl.multiple_of(b * 16, 16)
            partial[0, which, pl.ds(stats, 8), :] = folded(e)
            partial[0, which, pl.ds(stats + 8, 8), :] = folded(e * contract_last(v_ref[...], go))
            return carry

        lax.fori_loop(0, block_count(length), row_block, 0)


def prompt_kernel(
    meta, prompt, qs, gs, partial, ds_out, stats, prompt_grads,
    e_0, dp_0, e_1, dp_1, dk_acc, dv_acc,
):
    total = prompt.shape[0]
    head_dim = qs.shape[-1]
    rows = e_0.shape[1]
    buffers = ((e_0, dp_0), (e_1, dp_1))
    which = pl.program_id(1)
    length, seen = meta[2 * which], meta[2 * which + 1]

    @pl.when(which == 0)
    def _():
        dk_acc[...] = jnp.zeros(dk_acc.shape, jnp.float32)
        dv_acc[...] = jnp.zeros(dv_acc.shape, jnp.float32)

    def first_pass(low, high, b, e_s, dp_s):
        at = pl.ds(pl.multiple_of(b * rows, rows), rows)
        q, go = qs[0, 0, at, :], gs[0, 0, at, :]
        part = pl.multiple_of(b * 16, 16)
        sums = partial[0, 0, pl.ds(part, 8), :]
        dots = partial[0, 0, pl.ds(part + 8, 8), :]
        for base in range(0, high, KEY_CHUNK):
            chunk = slice(base, base + KEY_CHUNK)
            e = exponent(prompt[chunk, :head_dim], q)
            if base + KEY_CHUNK > low:
                index = lax.broadcasted_iota(jnp.int32, (KEY_CHUNK, rows), 0)
                e = jnp.where(index < seen - base, e, 0.0)
            dp = contract_last(prompt[chunk, head_dim:], go)
            e_s[chunk] = e
            dp_s[chunk] = dp
            sums += folded(e)
            dots += folded(e * dp)
        inverse = 1.0 / jnp.sum(sums, axis=0, keepdims=True)
        delta = jnp.sum(dots, axis=0, keepdims=True) * inverse
        stats[0, 0, pl.ds(part, 8), :] = jnp.broadcast_to(inverse, (8, rows))
        stats[0, 0, pl.ds(part + 8, 8), :] = jnp.broadcast_to(delta, (8, rows))
        return q, go, inverse, delta

    def second_pass(high, b, e_s, dp_s, q, go, inverse, delta):
        for base in range(0, high, KEY_CHUNK):
            chunk = slice(base, base + KEY_CHUNK)
            p = e_s[chunk] * inverse
            ds = (p * (dp_s[chunk] - delta)).astype(jnp.bfloat16)
            ds_out[0, 0, b, chunk, :] = ds
            dv_acc[chunk] += jnp.dot(
                p.astype(jnp.bfloat16), go, preferred_element_type=jnp.float32
            )
            dk_acc[chunk] += jnp.dot(ds, q, preferred_element_type=jnp.float32)

    def blocks(low, high):
        def run(some):
            held = [first_pass(low, high, b, *buffers[i]) for i, b in enumerate(some)]
            for i, b in enumerate(some):
                second_pass(high, b, *buffers[i], *held[i])

        def pair(i, carry):
            run((2 * i, 2 * i + 1))
            return carry

        count = block_count(length)
        lax.fori_loop(0, count // 2, pair, 0)

        @pl.when(count % 2 == 1)
        def _():
            run((count - 1,))

    step = total // KEY_STEPS
    for n in range(1, KEY_STEPS + 1):
        low, high = (n - 1) * step, n * step
        pl.when((seen > low) & (seen <= high))(functools.partial(blocks, low, high))

    @pl.when(which == pl.num_programs(1) - 1)
    def _():
        scale = head_dim ** (-0.5)
        prompt_grads[:, :head_dim] = (dk_acc[...] * scale).astype(jnp.bfloat16)
        prompt_grads[:, head_dim:] = dv_acc[...].astype(jnp.bfloat16)


def after_kernel(
    meta, q_own, k_own, v_own, q_other, k_other, v_other, prompt, qs, gs, ds_in, stats,
    q_gain, k_gain,
    dq_own, dk_own, dv_own, dq_other, dk_other, dv_other, dk_acc, dv_acc,
):
    slots, width = q_own.shape
    head_dim = k_own.shape[1]
    group = width // head_dim
    rows = ROW_SLOTS * group
    total = prompt.shape[0]
    scale = head_dim ** (-0.5)
    gain_q, gain_k = q_gain[...], k_gain[...]
    units = (
        (q_own, k_own, v_own, dq_own, dk_own, dv_own),
        (q_other, k_other, v_other, dq_other, dk_other, dv_other),
    )
    for which, (q_ref, k_ref, v_ref, dq_ref, dk_ref, dv_ref) in enumerate(units):
        length, seen = meta[2 * which], meta[2 * which + 1]
        key_x = k_ref[...].astype(jnp.float32)
        key_r, kn = head_norm(key_x, gain_k)
        dq_ref[...] = jnp.zeros(dq_ref.shape, dq_ref.dtype)
        dk_acc[...] = jnp.zeros(dk_acc.shape, jnp.float32)
        dv_acc[...] = jnp.zeros(dv_acc.shape, jnp.float32)

        def blocks(high, which=which, q_ref=q_ref, v_ref=v_ref, dq_ref=dq_ref, kn=kn, length=length):
            def row_block(b, carry):
                first = pl.multiple_of(b * ROW_SLOTS, ROW_SLOTS)
                at = pl.ds(pl.multiple_of(b * rows, rows), rows)
                q, go = qs[0, which, at, :], gs[0, which, at, :]
                part = pl.multiple_of(b * 16, 16)
                inverse = stats[0, which, pl.ds(part, 8), :][:1]
                delta = stats[0, which, pl.ds(part + 8, 8), :][:1]
                e = jnp.where(causal(slots, rows, first), exponent(kn, q), 0.0)
                p = e * inverse
                ds = (p * (contract_last(v_ref[...], go) - delta)).astype(jnp.bfloat16)
                dv_acc[...] += jnp.dot(
                    p.astype(jnp.bfloat16), go, preferred_element_type=jnp.float32
                )
                dk_acc[...] += jnp.dot(ds, q, preferred_element_type=jnp.float32)
                dq = contract_first(ds, kn) + contract_first(
                    ds_in[0, which, b, :high, :], prompt[:high, :head_dim]
                )
                dq = dq * scale
                for g in range(group):
                    cols = slice(g * head_dim, (g + 1) * head_dim)
                    x = q_ref[pl.ds(first, ROW_SLOTS), cols].astype(jnp.float32)
                    r = lax.rsqrt(jnp.mean(x * x, axis=-1, keepdims=True) + epsilon)
                    up = dq[g * ROW_SLOTS : (g + 1) * ROW_SLOTS]
                    dx = norm_backward(x, r, gain_q, up)
                    dq_ref[pl.ds(first, ROW_SLOTS), cols] = dx.astype(jnp.bfloat16)
                return carry

            lax.fori_loop(0, block_count(length), row_block, 0)

        step = total // KEY_STEPS
        for n in range(1, KEY_STEPS + 1):
            low, high = (n - 1) * step, n * step
            pl.when((seen > low) & (seen <= high))(functools.partial(blocks, high))
        dk = norm_backward(key_x, key_r, gain_k, dk_acc[...] * scale)
        dk_ref[...] = dk.astype(jnp.bfloat16)
        dv_ref[...] = dv_acc[...].astype(jnp.bfloat16)


def place_kernel(place, *refs):
    blocks, out = refs[:-1], refs[-1]
    for j, block in enumerate(blocks):
        out[lax.rem(place[0] + j, len(blocks))] = block[...]


def attend(heads, meta, own, other, prompt, weight_pair, q_gain, k_gain, width, head_dim):
    slots, total = own.shape[0], prompt.shape[0]
    group = width // head_dim
    rows = ROW_SLOTS * group
    steps = slots // ROW_SLOTS
    narrow = 2 * heads * group
    low, high = jnp.bfloat16, jnp.float32
    scalars = pl.BlockSpec(memory_space=pltpu.SMEM)
    gain = pl.BlockSpec((1, head_dim), lambda *i: (0, 0))

    def columns(block, index):
        return pl.BlockSpec((slots, block), lambda i, index=index: (0, index + i))

    def by_head(rows, block):
        return pl.BlockSpec((rows, block), lambda i, *_: (0, i))

    def by_pair(*shape):
        return pl.BlockSpec((1, 2, *shape), lambda i: (i, 0) + (0,) * len(shape))

    def by_unit(*shape):
        return pl.BlockSpec((1, 1, *shape), lambda i, k: (i, k) + (0,) * len(shape))

    def cost(products, keys, moved):
        return pl.CostEstimate(
            flops=heads * 2 * products * 2 * slots * group * keys * head_dim,
            bytes_accessed=moved,
            transcendentals=heads * 2 * slots * group * keys,
        )

    q_side = columns(width, 0)
    g_side = columns(width, heads)
    k_side = columns(head_dim, narrow)
    v_side = columns(head_dim, narrow + heads)
    stack, stat, shade = (steps * rows, head_dim), (steps * 16, rows), (steps, total, rows)

    def limit(mebibytes):
        return pltpu.CompilerParams(vmem_limit_bytes=mebibytes * 1024 * 1024)

    def shaped(shape, kind):
        return jax.ShapeDtypeStruct((heads, 2, *shape), kind)

    before = pl.pallas_call(
        before_kernel,
        grid=(heads,),
        in_specs=[scalars, q_side, g_side, k_side, v_side, q_side, g_side, k_side, v_side, gain, gain],
        out_specs=[by_pair(*stack), by_pair(*stack), by_pair(*stat)],
        out_shape=[shaped(stack, low), shaped(stack, low), shaped(stat, high)],
        compiler_params=limit(60),
        cost_estimate=cost(2, slots, 4 * 1024 * 1024),
    )
    qs, gs, partial = before(meta, own, own, own, own, other, other, other, other, q_gain, k_gain)
    prompt, qs, gs, partial = lax.optimization_barrier((prompt, qs, gs, partial))
    above, below = [], []
    for k in NEARBY:
        below.append(shifted(weight_pair, k))
        above.append(shifted(weight_pair, -k))
    middle = pl.pallas_call(
        prompt_kernel,
        grid=(heads, 2),
        in_specs=[scalars, by_head(total, 2 * head_dim), by_unit(*stack), by_unit(*stack), by_unit(*stat)],
        out_specs=[by_unit(*shade), by_unit(*stat), by_head(total, 2 * head_dim)],
        out_shape=[
            shaped(shade, low),
            shaped(stat, high),
            jax.ShapeDtypeStruct((total, heads * 2 * head_dim), low),
        ],
        scratch_shapes=[
            pltpu.VMEM((total, rows), high),
            pltpu.VMEM((total, rows), high),
            pltpu.VMEM((total, rows), high),
            pltpu.VMEM((total, rows), high),
            pltpu.VMEM((total, head_dim), high),
            pltpu.VMEM((total, head_dim), high),
        ],
        compiler_params=limit(57),
        cost_estimate=cost(4, total, 12 * 1024 * 1024),
    )
    ds, stats, prompt_grads = middle(meta, prompt, qs, gs, partial)
    outs = [(slots, width), (slots, head_dim), (slots, head_dim)] * 2
    last = pl.pallas_call(
        after_kernel,
        grid=(heads,),
        in_specs=[scalars, q_side, k_side, v_side, q_side, k_side, v_side]
        + [by_head(total, 2 * head_dim), by_pair(*stack), by_pair(*stack)]
        + [by_pair(*shade), by_pair(*stat), gain, gain],
        out_specs=[by_head(*s) for s in outs],
        out_shape=[jax.ShapeDtypeStruct((n, heads * m), low) for n, m in outs],
        scratch_shapes=[pltpu.VMEM((slots, head_dim), high), pltpu.VMEM((slots, head_dim), high)],
        compiler_params=limit(57),
        cost_estimate=cost(2, total, 14 * 1024 * 1024),
    )
    grads = last(
        meta, own, own, own, other, other, other, prompt, qs, gs, ds, stats, q_gain, k_gain
    )
    return (*grads, prompt_grads, [weight_pair, *above, *below])


def on_device(
    prompt_key_rows,
    prompt_value_rows,
    queries,
    keys,
    values,
    output_gradient,
    lengths,
    prompt_visible_rows,
    query_gain,
    key_norm_gain,
    key_value_weight,
):
    head_dim = query_gain.shape[0]
    core = lax.axis_index(PAIR)
    cores = lax.axis_size(PAIR)
    heads = keys.shape[1] // head_dim // cores
    narrow = heads * head_dim
    wide = queries.shape[1] // cores
    width = wide // heads
    near, far = lax.axis_size(NEAR), lax.axis_size(FAR)
    q_gain, k_gain = query_gain[None, :], key_norm_gain[None, :]

    def part(a, which, n):
        return lax.dynamic_slice_in_dim(a, which * n, n, axis=1)

    def in_core_order(mine, theirs):
        flip = core == 0
        return jnp.where(flip, mine, theirs), jnp.where(flip, theirs, mine)

    def prompt_part(which):
        return jnp.concatenate(
            [part(prompt_key_rows, which, narrow), part(prompt_value_rows, which, narrow)], axis=1
        )

    def pack(which):
        return jnp.concatenate(
            [
                part(queries, which, wide),
                part(output_gradient, which, wide),
                part(keys, which, narrow),
                part(values, which, narrow),
            ],
            axis=1,
        )

    def weight_part(which):
        cut = key_value_weight.reshape(-1, 2, cores, heads, head_dim)
        cut = lax.dynamic_index_in_dim(cut, which, 2, keepdims=False)
        return cut.transpose(0, 2, 1, 3).reshape(-1, 2 * narrow)

    raw = jnp.concatenate(in_core_order(prompt_part(core), swap(prompt_part(1 - core))), axis=0)
    count = raw.shape[0]
    px = raw[:, :narrow].astype(jnp.float32).reshape(count, heads, head_dim)
    pr = lax.rsqrt(jnp.mean(px * px, axis=-1, keepdims=True) + epsilon)
    pn = (px * pr * key_norm_gain).astype(jnp.bfloat16).reshape(count, narrow)
    pv = raw[:, narrow:]

    meta_own = jnp.stack([lengths[0], prompt_visible_rows[0]])
    meta = jnp.concatenate([meta_own, swap(meta_own)])
    own, other = pack(core), swap(pack(1 - core))
    weight_pair = jnp.concatenate(
        in_core_order(weight_part(core), swap(weight_part(1 - core))), axis=0
    )

    both = jnp.concatenate(
        [
            a[:, h * head_dim : (h + 1) * head_dim]
            for h in range(heads)
            for a in (pn, pv)
        ],
        axis=1,
    )
    prompt = from_everyone(both, PLANE).reshape(-1, 2 * narrow)

    results = attend(
        heads, meta, own, other, prompt, weight_pair, q_gain, k_gain, width, head_dim
    )

    sent, here, *arrived = lax.optimization_barrier((results[6], *results[7]))
    above, below = dict(zip(NEARBY, arrived[: len(NEARBY)])), dict(zip(NEARBY, arrived[len(NEARBY) :]))
    across = shifted(above[3], -1)
    ring = [here, above[1], above[2], above[3], across, below[3], below[2], below[1]]
    place = jnp.reshape(lax.axis_index(FAR), (1,))
    weight = pl.pallas_call(
        place_kernel,
        in_specs=[pl.BlockSpec(memory_space=pltpu.SMEM)]
        + [pl.BlockSpec(memory_space=pltpu.VMEM)] * far,
        out_specs=pl.BlockSpec(memory_space=pltpu.VMEM),
        out_shape=jax.ShapeDtypeStruct((far, *here.shape), here.dtype),
        compiler_params=pltpu.CompilerParams(vmem_limit_bytes=8 * 1024 * 1024),
        cost_estimate=pl.CostEstimate(
            flops=10**8, bytes_accessed=2 * far * here.size * 2, transcendentals=0
        ),
    )(place.astype(jnp.int32), *ring)
    weight = weight.reshape(-1, 2 * narrow)
    sent = sent.reshape(far * near, count, 2 * narrow)
    parts = lax.all_to_all(sent, PLANE, 0, 0, tiled=True)
    total = jnp.sum(parts.astype(jnp.float32), axis=0).reshape(count, heads, 2, head_dim)
    w = total[:, :, 0] * key_norm_gain
    inner = jnp.mean(w * px, axis=-1, keepdims=True)
    dk = pr * w - px * (pr * pr * pr) * inner
    grads = jnp.stack([dk, total[:, :, 1]], axis=2).reshape(count, 2 * narrow)
    rows = from_everyone(grads.astype(jnp.bfloat16), NEAR).reshape(-1, 2 * narrow)

    def assembled(index):
        return jnp.concatenate(in_core_order(results[index], swap(results[index + 3])), axis=1)

    query_grad, key_grad, value_grad = assembled(0), assembled(1), assembled(2)

    hidden = contract_last(rows, weight)
    per_core = count // cores
    hidden = hidden.reshape(near, cores, per_core, -1)
    mine = lax.dynamic_index_in_dim(hidden, core, 1, keepdims=False)
    theirs = lax.dynamic_index_in_dim(hidden, 1 - core, 1, keepdims=False)
    mine = (mine + swap(theirs.astype(jnp.bfloat16)).astype(jnp.float32)).astype(jnp.bfloat16)
    arrived = lax.all_to_all(mine, NEAR, 0, 0, tiled=True)
    arrived = arrived.reshape(near, per_core, far, -1)
    hidden_grad = arrived.transpose(1, 2, 0, 3).reshape(per_core, -1)
    return (query_grad, key_grad, value_grad, hidden_grad)


def solution(mesh):
    finer = Mesh(
        mesh.devices.reshape(mesh.shape["grp"], 8, 8, 2), ("grp", "cand_0", "cand_1", "cand_2")
    )
    return jax.shard_map(
        on_device,
        mesh=finer,
        in_specs=(
            P(GRP_CAND, None),
            P(GRP_CAND, None),
            P(GRP_CAND, None),
            P(GRP_CAND, None),
            P(GRP_CAND, None),
            P(GRP_CAND, None),
            P(GRP_CAND),
            P(GRP_CAND),
            P(),
            P(),
            P(CAND, None),
        ),
        out_specs=(P(GRP_CAND, None), P(GRP_CAND, None), P(GRP_CAND, None), P(GRP_CAND, None)),
        check_vma=False,
    )
```
